128 devices in a mesh: rows: 32 (over y, x, core), gz: 4 (over z).
Axes of the slice: x: 4, y: 4, z: 4, core: 2. Of those that a mesh axis runs over, the one named last changes fastest.
Arguments:
- segment_warming: float32 [64, 1024, 1024], P('gz', 'rows'), may hold values from 0.15 to 3
- eigenfunction_crosssections: float32 [10, 1024, 1024], P(None, 'rows'), may hold values from -2.5 to 2.5
- segment_phasors: float32 [64, 10], P('gz'), may hold values from 0.2 to 2
- injected_coefficients: float32 [2, 10], replicated, may hold values from -6 to 6
Outputs:
- diffused_warmth: float32 [64, 1024, 1024], P('gz', 'rows')
- refreshed_coupling_sums: float32 [64, 10, 10], P('gz')
- incoming_coefficients: float32 [64, 2, 10], P('gz')
The draws below stay inside these ranges and needn't reach their ends.
All inputs are finite; a program needn't handle non-finite values.
Results may differ from the reference program's by a relative error of at most 0.0003.
Values sent between devices are 32-bit elements; how exact they have to be, the bound alone decides.
No kernel may reach another device: no remote copies, remote signals or barrier semaphores. Data moves between devices by JAX's collectives and lax.ppermute only.
A program may use at most 128 MiB of HBM per device.

```python
import math
import jax
import jax.numpy as jnp
from jax import lax

NX = 1024
NY = 1024
M = 10
DIFFUSION_PASSES = 16
Z = 64


def transverse_grid():
    x_coord = (jnp.arange(NX, dtype=jnp.float32) + 0.5) * (2.0 / NX) - 1.0
    y_coord = (jnp.arange(NY, dtype=jnp.float32) + 0.5) * (2.0 / NY) - 1.0
    return (x_coord, y_coord)


def mode_orders(mode_count):
    order_pairs = []
    degree_sum = 0
    while len(order_pairs) < mode_count:
        for x_order in range(degree_sum, -1, -1):
            if len(order_pairs) < mode_count:
                order_pairs.append((x_order, degree_sum - x_order))
        degree_sum += 1
    return order_pairs


def hermite_table(coord, width, degree):
    scaled = coord / width
    polynomials = [jnp.ones_like(scaled), 2.0 * scaled]
    for level in range(1, degree):
        polynomials.append(2.0 * scaled * polynomials[level] - 2.0 * level * polynomials[level - 1])
    envelope = jnp.exp(-0.5 * scaled * scaled)
    return [poly_value * envelope for poly_value in polynomials[:degree + 1]]


def unit_power(shapes):
    return shapes / jnp.sqrt(jnp.mean(shapes * shapes, axis=(1, 2), keepdims=True))


def draw_eigenfunction_crosssections(key, part):
    x_coord, y_coord = transverse_grid()
    width_key = jax.random.fold_in(key, 11)
    mixing_key = jax.random.fold_in(key, 12)
    noise_key = jax.random.fold_in(key, 13)
    widths = jax.random.uniform(width_key, (2,), jnp.float32, 0.6, 0.8)
    strength = 0.35
    noise = 0.1 * jax.random.normal(noise_key, (M, NX, NY), jnp.float32)
    order_pairs = mode_orders(M)
    top_degree = max(1, max((max(order_pair) for order_pair in order_pairs)))
    x_table = hermite_table(x_coord, widths[0], top_degree)
    y_table = hermite_table(y_coord, widths[1], top_degree)
    shapes = jnp.stack([x_table[order_pair[0]][:, None] * y_table[order_pair[1]][None, :] for order_pair in order_pairs])
    shapes = unit_power(shapes)
    mixing = jnp.eye(M, dtype=jnp.float32) + strength * jax.random.normal(mixing_key, (M, M), jnp.float32)
    smooth = unit_power(jnp.einsum('mn,nxy->mxy', mixing, shapes, precision=lax.Precision.HIGHEST))
    noisy = smooth + noise
    peak = jnp.max(jnp.abs(noisy), axis=(1, 2), keepdims=True)
    return (2.5 * noisy / peak).astype(jnp.float32)


def draw_segment_warming(key, part):
    x_coord, y_coord = transverse_grid()
    wave_key = jax.random.fold_in(key, 21)
    phase_key = jax.random.fold_in(key, 22)
    noise_key = jax.random.fold_in(key, 23)
    tilt = 1.0 + 0.4 * x_coord
    strength = 0.5
    noise = jax.random.uniform(noise_key, (Z, NX, NY), jnp.float32, 0.6, 1.4)
    waves = jax.random.uniform(wave_key, (Z, 2), jnp.float32, 0.5, 3.0)
    phases = jax.random.uniform(phase_key, (Z,), jnp.float32, -math.pi, math.pi)
    argument = waves[:, 0, None, None] * x_coord[None, :, None] + waves[:, 1, None, None] * y_coord[None, None, :]
    grating = jnp.cos(math.pi * argument + phases[:, None, None])
    return (tilt[None, :, None] * (1.0 + strength * grating) * noise).astype(jnp.float32)


def level_of(stream_key, shape, pieces, least, largest):
    gain = 1.0
    for dim, shards_of in pieces:
        draws = jax.random.uniform(jax.random.fold_in(jax.random.fold_in(stream_key, 6), dim), (shards_of,), jnp.float32, least / len(pieces), largest / len(pieces))
        gain = gain * jnp.repeat(jnp.exp(draws), shape[dim] // shards_of).reshape((-1,) + (1,) * (len(shape) - 1 - dim))
    return gain


def normal_values(rng, shape, spread, bound, kind=jnp.bfloat16):
    return jnp.clip(spread * jax.random.normal(rng, shape, jnp.float32), -bound, bound).astype(kind)


def setup_inputs(seed: int = 0) -> dict:
    key_of = jax.random.split(jax.random.key(seed), 5)
    return {
        "segment_warming": draw_segment_warming(jax.random.fold_in(key_of[4], 71), 0),
        "eigenfunction_crosssections": draw_eigenfunction_crosssections(jax.random.fold_in(key_of[4], 71), 0),
        "segment_phasors": jnp.clip(jnp.exp(math.log(2.0) - 2.3025851 * jax.random.uniform(key_of[2], (Z, M), jnp.float32) ** level_of(key_of[2], (Z, M), ((0, 4),), -0.2, 0.2)), 0.2, 2.0),
        "injected_coefficients": normal_values(key_of[3], (2, M), 1.0, 6.0, jnp.float32),
    }


highest = lax.Precision.HIGHEST

def factor_entries(matrix):
    count = matrix.shape[-1]
    lower = [[None] * count for index in range(count)]
    for row in range(count):
        for column in range(row + 1):
            total = matrix[..., row, column]
            for inner in range(column):
                total = total - lower[row][inner] * lower[column][inner]
            if row == column:
                lower[row][column] = jnp.sqrt(total)
            else:
                lower[row][column] = total / lower[column][column]
    return lower

def cholesky_solve(lower, rhs):
    count = rhs.shape[-2]
    forward = []
    for row in range(count):
        total = rhs[..., row, :]
        for inner in range(row):
            total = total - lower[row][inner][..., None] * forward[inner]
        forward.append(total / lower[row][row][..., None])
    backward = [None] * count
    for row in range(count - 1, -1, -1):
        total = forward[row]
        for inner in range(row + 1, count):
            total = total - lower[inner][row][..., None] * backward[inner]
        backward[row] = total / lower[row][row][..., None]
    return jnp.stack(backward, axis=-2)

def propagators(constants, intersection_matrix):
    count = intersection_matrix.shape[-1]
    identity = jnp.eye(count, dtype=jnp.float32)
    doubled = intersection_matrix + jnp.swapaxes(intersection_matrix, -1, -2)
    coupled = doubled + identity * constants[..., None]
    squared = jnp.matmul(coupled, coupled, precision=highest)
    lower = factor_entries(identity + squared)
    return (cholesky_solve(lower, identity - squared), cholesky_solve(lower, 2.0 * coupled))

def rotate(matrix_real, matrix_imag, amplitude):
    real_amp = jnp.dot(matrix_real, amplitude[0], precision=highest) - jnp.dot(matrix_imag, amplitude[1], precision=highest)
    imag_amp = jnp.dot(matrix_real, amplitude[1], precision=highest) + jnp.dot(matrix_imag, amplitude[0], precision=highest)
    return jnp.stack([real_amp, imag_amp])

def march(matrices_real, matrices_imag, amplitude):

    def advance_one(carry, pair):
        return (rotate(pair[0], pair[1], carry), carry)
    final_amp, entrances = lax.scan(advance_one, amplitude, (matrices_real, matrices_imag))
    return entrances

def segment_coupling_sums(eigenfunction_crosssections, warmth_distribution):
    count = eigenfunction_crosssections.shape[0]
    flat = eigenfunction_crosssections.reshape(count, -1)
    weighted = (eigenfunction_crosssections * warmth_distribution[None]).reshape(count, -1)
    return jnp.dot(weighted, flat.T, precision=highest) / float(NX * NY)

def heat_source(eigenfunction_crosssections, amplitude):
    count = eigenfunction_crosssections.shape[0]
    flat = eigenfunction_crosssections.reshape(count, -1)
    field = jnp.einsum('zkm,mc->zkc', amplitude, flat, precision=highest)
    intensity = lax.optimization_barrier(jnp.sum(field * field, axis=1))
    return intensity.reshape((amplitude.shape[0],) + eigenfunction_crosssections.shape[1:])

def advance(padded, source):
    side_padded = jnp.pad(padded, ((0, 0), (0, 0), (1, 1)))
    center = side_padded[:, 1:-1, 1:-1]
    laplace = side_padded[:, 2:, 1:-1] + side_padded[:, :-2, 1:-1] + side_padded[:, 1:-1, 2:] + side_padded[:, 1:-1, :-2] - 4.0 * center
    return center + 0.2 * laplace + 0.01 * source

def reference(segment_warming, eigenfunction_crosssections, segment_phasors, injected_coefficients):
    beginning_value = lax.map(lambda warmth_distribution: segment_coupling_sums(eigenfunction_crosssections, warmth_distribution), segment_warming)
    matrices_real, matrices_imag = propagators(segment_phasors, beginning_value * 0.5 * 2.0)
    incoming_coefficients = march(matrices_real, matrices_imag, injected_coefficients)

    def advance_segment(pair):
        warmth_distribution, amplitude = pair
        source = heat_source(eigenfunction_crosssections, amplitude[None])
        field = warmth_distribution[None]
        for subcycle in range(DIFFUSION_PASSES):
            field = advance(jnp.pad(field, ((0, 0), (1, 1), (0, 0))), source)
        return (field[0], segment_coupling_sums(eigenfunction_crosssections, field[0]))
    diffused_warmth, refreshed_coupling_sums = lax.map(advance_segment, (segment_warming, incoming_coefficients))
    return (diffused_warmth, refreshed_coupling_sums, incoming_coefficients)
```

```python
import jax
import jax.numpy as jnp
import numpy as np
from jax import lax
from jax.experimental import pallas as pl
from jax.experimental.pallas import tpu as pltpu
from jax.sharding import PartitionSpec as P

NX = 1024
NY = 1024
M = 10
PASSES = 16
ROWS = 32
HALO = 16
WIDE = ROWS + 2 * HALO
ZL = 16
GZ = 4
TILES = NY // 128
BLOCK = 8
TALL = WIDE + BLOCK
highest = lax.Precision.HIGHEST
f32 = jnp.float32
bf16 = jnp.bfloat16


def pair_modes():
    table = []
    for group in range(8):
        for sub in range(8):
            if group < 3:
                table.append((group, sub))
            elif group == 3:
                table.append(((8, 8), (8, 9), (9, 9))[sub] if sub < 3 else (3, sub))
            elif group < 6:
                first = 4 + 2 * (group - 4)
                table.append((first, 4 + sub) if sub < 4 else (first + 1, sub))
            else:
                table.append((group + 2, sub))
    return table


def selection(stride, rows):
    where = {}
    for row, (m, n) in enumerate(pair_modes()):
        where.setdefault((m, n), row)
        where.setdefault((n, m), row)
    chosen = np.zeros((rows, 64), np.float32)
    for i in range(M):
        for j in range(M):
            chosen[i * stride + j, where[(i, j)]] = 1.0
    return chosen


def diagonal_rows():
    table = pair_modes()
    return [table.index((m, m)) for m in range(M)]


def split(value):
    high = value.astype(bf16)
    low = (value - high.astype(f32)).astype(bf16)
    return high, low


def pair_products(modes_ref, row):
    low = modes_ref[row, 0:8, :]
    sub = lax.broadcasted_iota(jnp.int32, (8, NY), 0)

    def mode(m):
        return jnp.broadcast_to(modes_ref[row, m : m + 1, :], (8, NY))

    m8, m9 = mode(8), mode(9)
    turned = jnp.where(sub < 4, pltpu.roll(low, 4, 0), low)
    left3 = jnp.where(sub < 2, m8, jnp.where(sub == 2, m9, mode(3)))
    right3 = jnp.where(sub == 0, m8, jnp.where(sub < 3, m9, low))
    groups = [
        mode(0) * low,
        mode(1) * low,
        mode(2) * low,
        left3 * right3,
        jnp.where(sub < 4, mode(4), mode(5)) * turned,
        jnp.where(sub < 4, mode(6), mode(7)) * turned,
        m8 * low,
        m9 * low,
    ]
    return jnp.concatenate(groups, axis=0)


def sums_of_rows(field_ref, modes_ref, first, unroll):
    def step(r, acc):
        products = jnp.concatenate(split(pair_products(modes_ref, first + r)), axis=0)
        warmth = jnp.concatenate(split(field_ref[first + r]), axis=0)
        return acc + lax.dot_general(
            products, warmth, (((1,), (1,)), ((), ())), preferred_element_type=f32
        )

    return lax.fori_loop(0, ROWS, step, jnp.zeros((128, 32), f32), unroll=unroll)


def packed_sums(acc, pad_ref, scale, extra):
    pad_ref[...] = jnp.zeros((128, 128), f32)
    pad_ref[:, 0:32] = acc
    both = pad_ref[0:64, :] + pad_ref[64:128, :]
    total = (both + pltpu.roll(both, 112, 1)) * scale
    lane = lax.broadcasted_iota(jnp.int32, (64, 128), 1)
    total = jnp.where(lane < ZL, total, 0.0)
    if extra is not None:
        total = total + extra
    packed = total[0:8]
    for group in range(1, 8):
        packed = packed + pltpu.roll(total[8 * group : 8 * group + 8], 16 * group, 1)
    return packed


def start_sums(w, e, ph, out, wt, et, pad, wsem, esem):
    copies = []
    for z in range(ZL):
        copies.append(pltpu.make_async_copy(w.at[z], wt.at[:, z, :], wsem.at[z]))
    for m in range(M):
        copies.append(pltpu.make_async_copy(e.at[m], et.at[:, m, :], esem.at[m]))
    for copy in copies:
        copy.start()
    pad[...] = jnp.zeros((128, 128), f32)
    pad[0:ZL, 0:M] = ph[...]
    turned = pad[...].T
    row = lax.broadcasted_iota(jnp.int32, (64, 128), 0)
    phases = jnp.zeros((64, 128), f32)
    for m, place in enumerate(diagonal_rows()):
        phases = phases + jnp.where(
            row == place, jnp.broadcast_to(turned[m : m + 1, :], (64, 128)), 0.0
        )
    phases = phases * jnp.where(lax.axis_index("rows") == 0, 1.0, 0.0)
    for copy in copies:
        copy.wait()
    acc = sums_of_rows(wt, et, 0, 16)
    packed = packed_sums(acc, pad, 2.0 / float(NX * NY), phases)
    out[...] = jnp.broadcast_to(packed[None], out.shape)


def three_parts(value):
    first = value.astype(bf16)
    rest = value - first.astype(f32)
    second = rest.astype(bf16)
    third = (rest - second.astype(f32)).astype(bf16)
    return jnp.concatenate([first, second, third], axis=0)


def lane_order():
    column = np.arange(NY)
    order = np.zeros((NY, NY), np.float32)
    order[column, (column % TILES) * 128 + column // TILES] = 1.0
    return order


def permuted(value, order_ref, back):
    count = value.shape[0]
    moved = lax.dot_general(
        three_parts(value),
        order_ref[...],
        (((1,), (1 if back else 0,)), ((), ())),
        preferred_element_type=f32,
    )
    return (moved[0:count] + moved[count : 2 * count]) + moved[2 * count :]


def reorder(w, e, order, unused, full, low, high, raw, moved, lsem, ssem):
    loads = [
        pltpu.make_async_copy(w, raw.at[0:ZL], lsem.at[0]),
        pltpu.make_async_copy(e, raw.at[ZL : ZL + M], lsem.at[1]),
    ]
    for copy in loads:
        copy.start()
    for copy in loads:
        copy.wait()
    stores = []
    for part, (start, stop) in enumerate(((0, 8), (8, 16), (16, 21), (21, 26))):
        rows = (stop - start) * ROWS
        block = raw[start:stop].reshape(rows, NY)
        moved[start:stop] = permuted(block, order, False).reshape(stop - start, ROWS, NY)
        here = slice(start, stop)
        stores += [
            pltpu.make_async_copy(
                moved.at[here, ROWS - HALO : ROWS, :], low.at[here], ssem.at[part, 0]
            ),
            pltpu.make_async_copy(moved.at[here, 0:HALO, :], high.at[here], ssem.at[part, 1]),
            pltpu.make_async_copy(moved.at[here], full.at[here], ssem.at[part, 2]),
        ]
        for copy in stores[-3:]:
            copy.start()
    for copy in stores:
        copy.wait()


def row_of(ref, *index):
    return jnp.broadcast_to(ref[index], (16, 128))


def amplitudes(parts, pick, v0, cs, ts, square, incoming):
    lane8 = lax.broadcasted_iota(jnp.int32, (8, 128), 1)
    totals = []
    for q in range(GZ):
        total = parts[q]
        for r in range(1, 32):
            total = total + parts[GZ * r + q]
        totals.append(total)
    rows = []
    for group in range(8):
        merged = jnp.zeros((8, 128), f32)
        for q in range(GZ):
            moved = pltpu.roll(totals[q], (16 * q - 16 * group) % 128, 1)
            merged = jnp.where(lane8 // ZL == q, moved, merged)
        rows.append(merged)
    pairs = jnp.concatenate(rows, axis=0)
    cs[...] = jnp.dot(pick[...], pairs, precision=highest, preferred_element_type=f32)

    sub = lax.broadcasted_iota(jnp.int32, (16, 128), 0)
    lane = lax.broadcasted_iota(jnp.int32, (16, 128), 1)
    coupled = [cs[16 * i : 16 * i + 16, :] for i in range(M)]
    matrix = []
    right = []
    for i in range(M):
        total = jnp.where(sub == i, 1.0, 0.0)
        for k in range(M):
            total = total + row_of(cs, pl.ds(16 * i + k, 1), slice(None)) * coupled[k]
        matrix.append(total)
        right.append(2.0 * coupled[i])
    for k in range(M):
        pivot = 1.0 / matrix[k][k : k + 1, :]
        pivot = jnp.broadcast_to(pivot, (16, 128))
        row_m = jnp.where(sub == k, pivot, matrix[k] * pivot)
        row_b = right[k] * pivot
        for i in range(M):
            if i != k:
                factor = jnp.broadcast_to(matrix[i][k : k + 1, :], (16, 128))
                matrix[i] = jnp.where(sub == k, 0.0, matrix[i]) - factor * row_m
                right[i] = right[i] - factor * row_b
        matrix[k] = row_m
        right[k] = row_b
    for i in range(M):
        ts[0, 0, 16 * i : 16 * i + 16, :] = 2.0 * matrix[i] - jnp.where(sub == i, 1.0, 0.0)
        ts[0, 1, 16 * i : 16 * i + 16, :] = right[i]

    for level in range(1, 6):
        back = 128 - (1 << (level - 1))
        later_r = [
            pltpu.roll(ts[level - 1, 0, 16 * j : 16 * j + 16, :], back, 1) for j in range(M)
        ]
        later_i = [
            pltpu.roll(ts[level - 1, 1, 16 * j : 16 * j + 16, :], back, 1) for j in range(M)
        ]
        for k in range(M):
            real = jnp.zeros((16, 128), f32)
            imag = jnp.zeros((16, 128), f32)
            for j in range(M):
                er = row_of(ts, level - 1, 0, pl.ds(16 * k + j, 1), slice(None))
                ei = row_of(ts, level - 1, 1, pl.ds(16 * k + j, 1), slice(None))
                real = real + (er * later_r[j] - ei * later_i[j])
                imag = imag + (er * later_i[j] + ei * later_r[j])
            ts[level, 0, 16 * k : 16 * k + 16, :] = real
            ts[level, 1, 16 * k : 16 * k + 16, :] = imag

    vr = jnp.zeros((16, 128), f32)
    vi = jnp.zeros((16, 128), f32)
    for m in range(M):
        spot = (sub == m) & (lane == 0)
        vr = jnp.where(spot, v0[0, m], vr)
        vi = jnp.where(spot, v0[1, m], vi)
    for level in range(5, -1, -1):
        half = 1 << level
        yr = jnp.zeros((16, 128), f32)
        yi = jnp.zeros((16, 128), f32)
        for k in range(M):
            tr = ts[level, 0, 16 * k : 16 * k + 16, :]
            ti = ts[level, 1, 16 * k : 16 * k + 16, :]
            ar = jnp.broadcast_to(vr[k : k + 1, :], (16, 128))
            ai = jnp.broadcast_to(vi[k : k + 1, :], (16, 128))
            yr = yr + (tr * ar - ti * ai)
            yi = yi + (tr * ai + ti * ar)
        target = lane % (2 * half) == half
        vr = jnp.where(target, pltpu.roll(yr, half, 1), vr)
        vi = jnp.where(target, pltpu.roll(yi, half, 1), vi)

    turn = (128 - ZL * lax.axis_index("gz")) % 128
    square[...] = jnp.zeros((128, 128), f32)
    vr = pltpu.roll(vr, turn, 1)
    vi = pltpu.roll(vi, turn, 1)
    incoming[:, 0, :] = vr[0:M, 0:ZL]
    incoming[:, 1, :] = vi[0:M, 0:ZL]
    square[0:16, :] = vr
    square[16:32, :] = vi
    turned = square[...].T[0:ZL, :]
    real = jnp.where(lane < 16, turned, 0.0)
    imag = jnp.where(lane < 16, pltpu.roll(turned, 112, 1), 0.0)
    return real, imag


def heat_load(real, imag, modes_ref, source_ref):
    both = jnp.concatenate([real, imag], axis=0)
    high = both.astype(bf16).astype(f32)
    low = both - high
    weights = high + pltpu.roll(high, 16, 1) + pltpu.roll(low, 32, 1) + pltpu.roll(low, 48, 1)
    weights = weights[:, 0:64].astype(bf16)

    def step(r, unused):
        high_e, low_e = split(modes_ref[r])
        stacked = jnp.concatenate([high_e, low_e, high_e, low_e], axis=0)
        field = jnp.dot(weights, stacked, preferred_element_type=f32)
        re, im = field[0:16], field[16:32]
        source_ref[r] = 0.01 * (re * re + im * im)
        return unused

    lax.fori_loop(0, WIDE, step, 0, unroll=16)


def one_pass(old, new, source, number):
    lane = lax.broadcasted_iota(jnp.int32, (8, 128), 1)
    first_lane = lane == 0
    last_lane = lane == 127

    def block(b, unused):
        r = number + BLOCK * b
        for half in range(2):
            z = slice(8 * half, 8 * half + 8)
            rows = [
                [old[r - 1 + i, z, 128 * t : 128 * t + 128] for t in range(TILES)]
                for i in range(BLOCK + 2)
            ]
            for i in range(BLOCK):
                center = rows[i + 1]
                before = jnp.where(first_lane, 0.0, pltpu.roll(center[TILES - 1], 1, 1))
                after = jnp.where(last_lane, 0.0, pltpu.roll(center[0], 127, 1))
                for t in range(TILES):
                    left = center[t - 1] if t else before
                    right = center[t + 1] if t < TILES - 1 else after
                    total = (rows[i][t] + center[t]) + (rows[i + 2][t] + (left + right))
                    cut = slice(128 * t, 128 * t + 128)
                    new[r + i, z, cut] = 0.2 * total + source[r + i, z, cut]
        return unused

    lax.fori_loop(0, (WIDE - 2 * number + BLOCK - 1) // BLOCK, block, 0)


def heat_and_sums(
    parts, fields, above, below, pick, order, v0,
    field, out, incoming,
    f0, f1, source, et, cs, ts, square, wsem, esem, osem,
):
    copies = []
    for z in range(ZL):
        copies += [
            pltpu.make_async_copy(fields.at[z], f0.at[HALO : HALO + ROWS, z, :], wsem.at[0, z]),
            pltpu.make_async_copy(above.at[z], f0.at[0:HALO, z, :], wsem.at[1, z]),
            pltpu.make_async_copy(below.at[z], f0.at[HALO + ROWS : WIDE, z, :], wsem.at[2, z]),
        ]
    mode_copies = []
    for m in range(M):
        j = ZL + m
        mode_copies += [
            pltpu.make_async_copy(fields.at[j], et.at[HALO : HALO + ROWS, m, :], esem.at[0, m]),
            pltpu.make_async_copy(above.at[j], et.at[0:HALO, m, :], esem.at[1, m]),
            pltpu.make_async_copy(below.at[j], et.at[HALO + ROWS : WIDE, m, :], esem.at[2, m]),
        ]
    et[:, 8:16, :] = jnp.zeros((WIDE, 8, NY), f32)
    for copy in mode_copies:
        copy.start()
    for copy in copies:
        copy.start()
    real, imag = amplitudes(parts, pick, v0, cs, ts, square, incoming)
    for copy in mode_copies:
        copy.wait()
    heat_load(real, imag, et, source)
    for copy in copies:
        copy.wait()
    place = lax.axis_index("rows")
    first = place == 0
    last = place == lax.axis_size("rows") - 1
    buffers = (f0, f1)
    for number in range(1, PASSES + 1):
        old, new = buffers[(number - 1) % 2], buffers[number % 2]
        one_pass(old, new, source, number)
        if number < PASSES:

            @pl.when(first)
            def _():
                new[HALO - 1] = jnp.zeros((ZL, NY), f32)

            @pl.when(last)
            def _():
                new[HALO + ROWS] = jnp.zeros((ZL, NY), f32)

    done, plain = buffers[PASSES % 2], buffers[1 - PASSES % 2]
    outs = []
    for part in range(ROWS // 8):
        at = slice(8 * part, 8 * part + 8)
        block = done[HALO + 8 * part : HALO + 8 * part + 8].reshape(8 * ZL, NY)
        plain[at] = permuted(block, order, True).reshape(8, ZL, NY)
        for z in range(ZL):
            copy = pltpu.make_async_copy(plain.at[at, z, :], field.at[z, at, :], osem.at[part, z])
            copy.start()
            outs.append(copy)
    acc = sums_of_rows(done, et, HALO, 16)
    packed = packed_sums(acc, square, 1.0 / float(NX * NY), None)
    out[...] = jnp.broadcast_to(packed[None], out.shape)
    for copy in outs:
        copy.wait()


def spread(parts, pick, out):
    total = parts[0]
    for r in range(1, parts.shape[0]):
        total = total + parts[r]
    rows = [total] + [pltpu.roll(total, 128 - 16 * group, 1) for group in range(1, 8)]
    pairs = jnp.concatenate(rows, axis=0)
    table = jnp.dot(pick[...], pairs, precision=highest, preferred_element_type=f32).T
    for m in range(M):
        out[m] = table[0:ZL, M * m : M * m + M]


def shards(segment_warming, eigenfunction_crosssections, segment_phasors, injected_coefficients):
    devices = lax.axis_size("rows")
    hbm = pl.BlockSpec(memory_space=pl.ANY)
    vmem = pl.BlockSpec(memory_space=pltpu.VMEM)
    smem = pl.BlockSpec(memory_space=pltpu.SMEM)
    dma = pltpu.SemaphoreType.DMA
    edge = jax.ShapeDtypeStruct((ZL + M, HALO, NY), f32)
    both = jax.ShapeDtypeStruct((ZL + M, ROWS, NY), f32)
    order = jnp.asarray(lane_order(), dtype=bf16)
    packed = pl.pallas_call(
        start_sums,
        name="start_sums",
        out_shape=jax.ShapeDtypeStruct((devices * GZ, 8, 128), f32),
        in_specs=[hbm, hbm, vmem],
        out_specs=vmem,
        scratch_shapes=[
            pltpu.VMEM((ROWS, ZL, NY), f32),
            pltpu.VMEM((ROWS, 16, NY), f32),
            pltpu.VMEM((128, 128), f32),
            dma((ZL,)),
            dma((M,)),
        ],
        compiler_params=pltpu.CompilerParams(vmem_limit_bytes=16 << 20),
    )(segment_warming, eigenfunction_crosssections, segment_phasors)
    parts = lax.all_to_all(packed, ("rows", "gz"), 0, 0, tiled=True)
    fields, low, high = pl.pallas_call(
        reorder,
        name="reorder",
        out_shape=(both, edge, edge),
        in_specs=[hbm, hbm, vmem, hbm],
        out_specs=(hbm, hbm, hbm),
        scratch_shapes=[
            pltpu.VMEM((ZL + M, ROWS, NY), f32),
            pltpu.VMEM((ZL + M, ROWS, NY), f32),
            dma((2,)),
            dma((4, 3)),
        ],
        cost_estimate=pl.CostEstimate(
            flops=6 * (ZL + M) * ROWS * NY * NY, bytes_accessed=14 << 20, transcendentals=0
        ),
        compiler_params=pltpu.CompilerParams(vmem_limit_bytes=32 << 20),
    )(segment_warming, eigenfunction_crosssections, order, packed)
    forward = [(i, i + 1) for i in range(devices - 1)]
    backward = [(target, origin) for origin, target in forward]
    above = lax.ppermute(low, "rows", forward)
    below = lax.ppermute(high, "rows", backward)
    field, packed, incoming = pl.pallas_call(
        heat_and_sums,
        name="heat_and_sums",
        out_shape=(
            jax.ShapeDtypeStruct((ZL, ROWS, NY), f32),
            jax.ShapeDtypeStruct((devices, 8, 128), f32),
            jax.ShapeDtypeStruct((M, 2, ZL), f32),
        ),
        in_specs=[vmem, hbm, hbm, hbm, vmem, vmem, smem],
        out_specs=(hbm, vmem, vmem),
        scratch_shapes=[
            pltpu.VMEM((TALL, ZL, NY), f32),
            pltpu.VMEM((TALL, ZL, NY), f32),
            pltpu.VMEM((TALL, ZL, NY), f32),
            pltpu.VMEM((WIDE, 16, NY), f32),
            pltpu.VMEM((160, 128), f32),
            pltpu.VMEM((6, 2, 160, 128), f32),
            pltpu.VMEM((128, 128), f32),
            dma((3, ZL)),
            dma((3, M)),
            dma((ROWS // 8, ZL)),
        ],
        compiler_params=pltpu.CompilerParams(vmem_limit_bytes=40 << 20),
    )(
        parts,
        fields,
        above,
        below,
        jnp.asarray(selection(16, 160)),
        order,
        injected_coefficients,
    )
    parts = lax.all_to_all(packed, "rows", 0, 0, tiled=True)
    refreshed = pl.pallas_call(
        spread,
        name="spread",
        out_shape=jax.ShapeDtypeStruct((M, ZL, M), f32),
        in_specs=[vmem, vmem],
        out_specs=vmem,
        compiler_params=pltpu.CompilerParams(vmem_limit_bytes=8 << 20),
    )(parts, jnp.asarray(selection(M, 128)))
    return (field, jnp.transpose(refreshed, (1, 0, 2)), jnp.transpose(incoming, (2, 1, 0)))


def solution(mesh):
    placed = (P("gz", "rows", None), P(None, "rows", None), P("gz", None), P())
    return jax.shard_map(
        shards,
        mesh=mesh,
        in_specs=placed,
        out_specs=(P("gz", "rows", None), P("gz", None, None), P("gz", None, None)),
        check_vma=False,
    )
```

```python
import jax
import jax.numpy as jnp
import numpy as np
from jax import lax
from jax.experimental import pallas as pl
from jax.experimental.pallas import tpu as pltpu
from jax.sharding import PartitionSpec as P

NX = 1024
NY = 1024
M = 10
PASSES = 16
ROWS = 32
HALO = 16
WIDE = ROWS + 2 * HALO
ZL = 16
GZ = 4
TILES = NY // 128
BLOCK = 8
TALL = WIDE + BLOCK
highest = lax.Precision.HIGHEST
f32 = jnp.float32
bf16 = jnp.bfloat16


def pair_modes():
    table = []
    for group in range(8):
        for sub in range(8):
            if group < 3:
                table.append((group, sub))
            elif group == 3:
                table.append(((8, 8), (8, 9), (9, 9))[sub] if sub < 3 else (3, sub))
            elif group < 6:
                first = 4 + 2 * (group - 4)
                table.append((first, 4 + sub) if sub < 4 else (first + 1, sub))
            else:
                table.append((group + 2, sub))
    return table


def selection(stride, rows):
    where = {}
    for row, (m, n) in enumerate(pair_modes()):
        where.setdefault((m, n), row)
        where.setdefault((n, m), row)
    chosen = np.zeros((rows, 64), np.float32)
    for i in range(M):
        for j in range(M):
            chosen[i * stride + j, where[(i, j)]] = 1.0
    return chosen


def diagonal_rows():
    table = pair_modes()
    return [table.index((m, m)) for m in range(M)]


def split(value):
    high = value.astype(bf16)
    low = (value - high.astype(f32)).astype(bf16)
    return high, low


def pair_products(modes_ref, row):
    low = modes_ref[row, 0:8, :]
    sub = lax.broadcasted_iota(jnp.int32, (8, NY), 0)

    def mode(m):
        return jnp.broadcast_to(modes_ref[row, m : m + 1, :], (8, NY))

    m8, m9 = mode(8), mode(9)
    turned = jnp.where(sub < 4, pltpu.roll(low, 4, 0), low)
    left3 = jnp.where(sub < 2, m8, jnp.where(sub == 2, m9, mode(3)))
    right3 = jnp.where(sub == 0, m8, jnp.where(sub < 3, m9, low))
    groups = [
        mode(0) * low,
        mode(1) * low,
        mode(2) * low,
        left3 * right3,
        jnp.where(sub < 4, mode(4), mode(5)) * turned,
        jnp.where(sub < 4, mode(6), mode(7)) * turned,
        m8 * low,
        m9 * low,
    ]
    return jnp.concatenate(groups, axis=0)


def sums_of_rows(field_ref, first, modes_ref, modes_first, count, unroll, start):
    def step(r, acc):
        products = jnp.concatenate(split(pair_products(modes_ref, modes_first + r)), axis=0)
        warmth = jnp.concatenate(split(field_ref[first + r]), axis=0)
        return acc + lax.dot_general(
            products, warmth, (((1,), (1,)), ((), ())), preferred_element_type=f32
        )

    return lax.fori_loop(0, count, step, start, unroll=unroll)


def packed_sums(acc, pad_ref, scale, extra):
    pad_ref[...] = jnp.zeros((128, 128), f32)
    pad_ref[:, 0:32] = acc
    both = pad_ref[0:64, :] + pad_ref[64:128, :]
    total = (both + pltpu.roll(both, 112, 1)) * scale
    lane = lax.broadcasted_iota(jnp.int32, (64, 128), 1)
    total = jnp.where(lane < ZL, total, 0.0)
    if extra is not None:
        total = total + extra
    packed = total[0:8]
    for group in range(1, 8):
        packed = packed + pltpu.roll(total[8 * group : 8 * group + 8], 16 * group, 1)
    return packed


def start_sums(w, e, ph, out, low, high, wt, et, pad, wsem, esem, hsem):
    half = ROWS // 2
    chunks, edges = [], []
    for part, edge in enumerate((high, low)):
        at = slice(half * part, half * (part + 1))
        chunks.append(
            [
                pltpu.make_async_copy(e.at[m, at, :], et.at[at, m, :], esem.at[part, m])
                for m in range(M)
            ]
            + [
                pltpu.make_async_copy(w.at[z, at, :], wt.at[at, z, :], wsem.at[part, z])
                for z in range(ZL)
            ]
        )
        edges += [
            pltpu.make_async_copy(wt.at[at, z, :], edge.at[z], hsem.at[part, z]) for z in range(ZL)
        ] + [
            pltpu.make_async_copy(et.at[at, m, :], edge.at[ZL + m], hsem.at[part, ZL + m])
            for m in range(M)
        ]
    for copies in chunks:
        for copy in copies:
            copy.start()
    pad[...] = jnp.zeros((128, 128), f32)
    pad[0:ZL, 0:M] = ph[...]
    turned = pad[...].T
    row = lax.broadcasted_iota(jnp.int32, (64, 128), 0)
    phases = jnp.zeros((64, 128), f32)
    for m, place in enumerate(diagonal_rows()):
        phases = phases + jnp.where(
            row == place, jnp.broadcast_to(turned[m : m + 1, :], (64, 128)), 0.0
        )
    phases = phases * jnp.where(lax.axis_index("rows") == 0, 1.0, 0.0)
    acc = jnp.zeros((128, 32), f32)
    for part, copies in enumerate(chunks):
        for copy in copies:
            copy.wait()
        for copy in edges[(ZL + M) * part : (ZL + M) * (part + 1)]:
            copy.start()
        acc = sums_of_rows(wt, half * part, et, half * part, half, 16, acc)
    packed = packed_sums(acc, pad, 2.0 / float(NX * NY), phases)
    out[...] = jnp.broadcast_to(packed[None], out.shape)
    for copy in edges:
        copy.wait()


def spots(k):
    return pl.ds(64 * (k % 2) + k // 2, 8, stride=8)


def turn_in(value, new, row):
    stacked = jnp.concatenate([value[:, 128 * t : 128 * t + 128] for t in range(TILES)], axis=0)
    across = stacked.T
    for k in range(16):
        new[row, spots(k), :] = across[8 * k : 8 * k + 8]


def turn_out(old, row, new, new_row):
    across = jnp.concatenate([old[row, spots(k), :] for k in range(16)], axis=0).T
    for t in range(TILES):
        new[new_row, :, 128 * t : 128 * t + 128] = across[16 * t : 16 * t + 16]


def turn_warming(w, above, below, unused, out, raw, new, lsem, ssem):
    sides = (
        (w, HALO, ROWS),
        (above, 0, HALO),
        (below, HALO + ROWS, HALO),
    )
    loads, stores = [], []
    for side, (origin, start, count) in enumerate(sides):
        at = slice(start, start + count)
        loads.append(
            [
                pltpu.make_async_copy(origin.at[z], raw.at[at, z, :], lsem.at[side, z])
                for z in range(ZL)
            ]
        )
        stores.append(pltpu.make_async_copy(new.at[at], out.at[at], ssem.at[side]))
        for copy in loads[side]:
            copy.start()
    for side, (origin, start, count) in enumerate(sides):
        for copy in loads[side]:
            copy.wait()

        def step(r, unused):
            turn_in(raw[start + r], new, start + r)
            return unused

        lax.fori_loop(0, count, step, 0, unroll=8)
        stores[side].start()
    for copy in stores:
        copy.wait()


def row_of(ref, *index):
    return jnp.broadcast_to(ref[index], (16, 128))


def amplitudes(parts, pick, v0, cs, ts, square, incoming):
    lane8 = lax.broadcasted_iota(jnp.int32, (8, 128), 1)
    totals = []
    for q in range(GZ):
        total = parts[q]
        for r in range(1, 32):
            total = total + parts[GZ * r + q]
        totals.append(total)
    rows = []
    for group in range(8):
        merged = jnp.zeros((8, 128), f32)
        for q in range(GZ):
            moved = pltpu.roll(totals[q], (16 * q - 16 * group) % 128, 1)
            merged = jnp.where(lane8 // ZL == q, moved, merged)
        rows.append(merged)
    pairs = jnp.concatenate(rows, axis=0)
    cs[...] = jnp.dot(pick[...], pairs, precision=highest, preferred_element_type=f32)

    sub = lax.broadcasted_iota(jnp.int32, (16, 128), 0)
    lane = lax.broadcasted_iota(jnp.int32, (16, 128), 1)
    coupled = [cs[16 * i : 16 * i + 16, :] for i in range(M)]
    matrix = []
    right = []
    for i in range(M):
        total = jnp.where(sub == i, 1.0, 0.0)
        for k in range(M):
            total = total + row_of(cs, pl.ds(16 * i + k, 1), slice(None)) * coupled[k]
        matrix.append(total)
        right.append(2.0 * coupled[i])
    for k in range(M):
        pivot = 1.0 / matrix[k][k : k + 1, :]
        pivot = jnp.broadcast_to(pivot, (16, 128))
        row_m = jnp.where(sub == k, pivot, matrix[k] * pivot)
        row_b = right[k] * pivot
        for i in range(M):
            if i != k:
                factor = jnp.broadcast_to(matrix[i][k : k + 1, :], (16, 128))
                matrix[i] = jnp.where(sub == k, 0.0, matrix[i]) - factor * row_m
                right[i] = right[i] - factor * row_b
        matrix[k] = row_m
        right[k] = row_b
    for i in range(M):
        ts[0, 0, 16 * i : 16 * i + 16, :] = 2.0 * matrix[i] - jnp.where(sub == i, 1.0, 0.0)
        ts[0, 1, 16 * i : 16 * i + 16, :] = right[i]

    for level in range(1, 6):
        back = 128 - (1 << (level - 1))
        later_r = [
            pltpu.roll(ts[level - 1, 0, 16 * j : 16 * j + 16, :], back, 1) for j in range(M)
        ]
        later_i = [
            pltpu.roll(ts[level - 1, 1, 16 * j : 16 * j + 16, :], back, 1) for j in range(M)
        ]
        for k in range(M):
            real = jnp.zeros((16, 128), f32)
            imag = jnp.zeros((16, 128), f32)
            for j in range(M):
                er = row_of(ts, level - 1, 0, pl.ds(16 * k + j, 1), slice(None))
                ei = row_of(ts, level - 1, 1, pl.ds(16 * k + j, 1), slice(None))
                real = real + (er * later_r[j] - ei * later_i[j])
                imag = imag + (er * later_i[j] + ei * later_r[j])
            ts[level, 0, 16 * k : 16 * k + 16, :] = real
            ts[level, 1, 16 * k : 16 * k + 16, :] = imag

    vr = jnp.zeros((16, 128), f32)
    vi = jnp.zeros((16, 128), f32)
    for m in range(M):
        spot = (sub == m) & (lane == 0)
        vr = jnp.where(spot, v0[0, m], vr)
        vi = jnp.where(spot, v0[1, m], vi)
    for level in range(5, -1, -1):
        half = 1 << level
        yr = jnp.zeros((16, 128), f32)
        yi = jnp.zeros((16, 128), f32)
        for k in range(M):
            tr = ts[level, 0, 16 * k : 16 * k + 16, :]
            ti = ts[level, 1, 16 * k : 16 * k + 16, :]
            ar = jnp.broadcast_to(vr[k : k + 1, :], (16, 128))
            ai = jnp.broadcast_to(vi[k : k + 1, :], (16, 128))
            yr = yr + (tr * ar - ti * ai)
            yi = yi + (tr * ai + ti * ar)
        target = lane % (2 * half) == half
        vr = jnp.where(target, pltpu.roll(yr, half, 1), vr)
        vi = jnp.where(target, pltpu.roll(yi, half, 1), vi)

    turn = (128 - ZL * lax.axis_index("gz")) % 128
    square[...] = jnp.zeros((128, 128), f32)
    vr = pltpu.roll(vr, turn, 1)
    vi = pltpu.roll(vi, turn, 1)
    incoming[:, 0, :] = vr[0:M, 0:ZL]
    incoming[:, 1, :] = vi[0:M, 0:ZL]
    square[0:16, :] = vr
    square[16:32, :] = vi
    turned = square[...].T[0:ZL, :]
    real = jnp.where(lane < 16, turned, 0.0)
    imag = jnp.where(lane < 16, pltpu.roll(turned, 112, 1), 0.0)
    return real, imag


def heat_load(real, imag, modes_ref, source_ref):
    both = jnp.concatenate([real, imag], axis=0)
    high = both.astype(bf16).astype(f32)
    low = both - high
    weights = high + pltpu.roll(high, 16, 1) + pltpu.roll(low, 32, 1) + pltpu.roll(low, 48, 1)
    weights = weights[:, 0:64].astype(bf16)

    def step(r, unused):
        high_e, low_e = split(modes_ref[r])
        stacked = jnp.concatenate([high_e, low_e, high_e, low_e], axis=0)
        field = jnp.dot(weights, stacked, preferred_element_type=f32)
        re, im = field[0:16], field[16:32]
        turn_in(0.01 * (re * re + im * im), source_ref, r)
        return unused

    lax.fori_loop(0, WIDE, step, 0, unroll=16)


def one_pass(old, new, source, number):
    lane = lax.broadcasted_iota(jnp.int32, (8, 128), 1)
    sub = lax.broadcasted_iota(jnp.int32, (8, 128), 0)

    def block(b, unused):
        r = number + BLOCK * b
        for half in range(2):
            some = range(8 * half, 8 * half + 8)

            def register(row, v):
                return old[row, 8 * v : 8 * v + 8, :]

            rows = [{v: register(r - 1 + i, v) for v in some} for i in range(BLOCK + 2)]
            for i in range(BLOCK):
                center = dict(rows[i + 1])
                if half == 0:
                    near = pltpu.roll(register(r + i, 15), 1, 0)
                    far = jnp.where(lane < 16, 0.0, pltpu.roll(near, 16, 1))
                    center[-1] = jnp.where(sub == 0, far, near)
                    center[8] = register(r + i, 8)
                else:
                    near = pltpu.roll(register(r + i, 0), 7, 0)
                    far = jnp.where(lane >= 112, 0.0, pltpu.roll(near, 112, 1))
                    center[16] = jnp.where(sub == 7, far, near)
                    center[7] = register(r + i, 7)
                for v in some:
                    sides = center[v - 1] + center[v + 1]
                    total = (rows[i][v] + center[v]) + (rows[i + 2][v] + sides)
                    cut = slice(8 * v, 8 * v + 8)
                    new[r + i, cut, :] = 0.2 * total + source[r + i, cut, :]
        return unused

    lax.fori_loop(0, (WIDE - 2 * number + BLOCK - 1) // BLOCK, block, 0)


def heat_and_sums(
    parts, warm, e, edge_above, edge_below, pick, v0,
    field, out, incoming,
    f0, f1, source, et, plain, cs, ts, square, wsem, esem, osem,
):
    warm_copy = pltpu.make_async_copy(warm, f0.at[0:WIDE], wsem)
    mode_copies = []
    for m in range(M):
        for side, (origin, at) in enumerate(
            (
                (e.at[m], slice(HALO, HALO + ROWS)),
                (edge_above.at[ZL + m], slice(0, HALO)),
                (edge_below.at[ZL + m], slice(HALO + ROWS, WIDE)),
            )
        ):
            mode_copies.append(pltpu.make_async_copy(origin, et.at[at, m, :], esem.at[side, m]))
    et[:, 8:16, :] = jnp.zeros((WIDE, 8, NY), f32)
    for copy in mode_copies:
        copy.start()
    warm_copy.start()
    real, imag = amplitudes(parts, pick, v0, cs, ts, square, incoming)
    for copy in mode_copies:
        copy.wait()
    heat_load(real, imag, et, source)
    warm_copy.wait()
    place = lax.axis_index("rows")
    first = place == 0
    last = place == lax.axis_size("rows") - 1
    buffers = (f0, f1)
    for number in range(1, PASSES + 1):
        old, new = buffers[(number - 1) % 2], buffers[number % 2]
        one_pass(old, new, source, number)
        if number < PASSES:

            @pl.when(first)
            def _():
                new[HALO - 1] = jnp.zeros((128, 128), f32)

            @pl.when(last)
            def _():
                new[HALO + ROWS] = jnp.zeros((128, 128), f32)

    done = buffers[PASSES % 2]
    outs = []
    for part in range(ROWS // 8):
        at = slice(8 * part, 8 * part + 8)
        for r in range(8 * part, 8 * part + 8):
            turn_out(done, HALO + r, plain, r)
        for z in range(ZL):
            copy = pltpu.make_async_copy(plain.at[at, z, :], field.at[z, at, :], osem.at[part, z])
            copy.start()
            outs.append(copy)
    acc = sums_of_rows(plain, 0, et, HALO, ROWS, 16, jnp.zeros((128, 32), f32))
    packed = packed_sums(acc, square, 1.0 / float(NX * NY), None)
    out[...] = jnp.broadcast_to(packed[None], out.shape)
    for copy in outs:
        copy.wait()


def spread(parts, pick, out):
    total = parts[0]
    for r in range(1, parts.shape[0]):
        total = total + parts[r]
    rows = [total] + [pltpu.roll(total, 128 - 16 * group, 1) for group in range(1, 8)]
    pairs = jnp.concatenate(rows, axis=0)
    table = jnp.dot(pick[...], pairs, precision=highest, preferred_element_type=f32).T
    for m in range(M):
        out[m] = table[0:ZL, M * m : M * m + M]


def on_hbm(array):
    return pltpu.with_memory_space_constraint(array, pltpu.HBM)


def shards(segment_warming, eigenfunction_crosssections, segment_phasors, injected_coefficients):
    devices = lax.axis_size("rows")
    hbm = pl.BlockSpec(memory_space=pltpu.HBM)
    vmem = pl.BlockSpec(memory_space=pltpu.VMEM)
    smem = pl.BlockSpec(memory_space=pltpu.SMEM)
    dma = pltpu.SemaphoreType.DMA
    edge = pltpu.HBM((ZL + M, HALO, NY), f32)
    slab_vmem = pltpu.VMEM((ROWS, 16, NY), f32)
    warming, shapes = on_hbm(segment_warming), on_hbm(eigenfunction_crosssections)
    packed, low, high = pl.pallas_call(
        start_sums,
        name="start_sums",
        out_shape=(jax.ShapeDtypeStruct((devices * GZ, 8, 128), f32), edge, edge),
        in_specs=[hbm, hbm, vmem],
        out_specs=(vmem, hbm, hbm),
        scratch_shapes=[
            slab_vmem,
            slab_vmem,
            pltpu.VMEM((128, 128), f32),
            dma((2, ZL)),
            dma((2, M)),
            dma((2, ZL + M)),
        ],
        compiler_params=pltpu.CompilerParams(vmem_limit_bytes=16 << 20),
    )(warming, shapes, segment_phasors)
    forward = [(i, i + 1) for i in range(devices - 1)]
    backward = [(target, origin) for origin, target in forward]
    above = lax.ppermute(low, "rows", forward)
    below = lax.ppermute(high, "rows", backward)
    parts = lax.all_to_all(packed, ("rows", "gz"), 0, 0, tiled=True)
    warm = pl.pallas_call(
        turn_warming,
        name="turn_warming",
        out_shape=pltpu.HBM((WIDE, 128, 128), f32),
        in_specs=[hbm, hbm, hbm, pl.BlockSpec(memory_space=pl.ANY)],
        out_specs=hbm,
        scratch_shapes=[
            pltpu.VMEM((WIDE, ZL, NY), f32),
            pltpu.VMEM((WIDE, 128, 128), f32),
            dma((3, ZL)),
            dma((3,)),
        ],
        compiler_params=pltpu.CompilerParams(vmem_limit_bytes=16 << 20),
    )(warming, on_hbm(above), on_hbm(below), packed)
    wide_vmem = pltpu.VMEM((TALL, 128, 128), f32)
    field, packed, incoming = pl.pallas_call(
        heat_and_sums,
        name="heat_and_sums",
        out_shape=(
            jax.ShapeDtypeStruct((ZL, ROWS, NY), f32),
            jax.ShapeDtypeStruct((devices, 8, 128), f32),
            jax.ShapeDtypeStruct((M, 2, ZL), f32),
        ),
        in_specs=[vmem, hbm, hbm, hbm, hbm, vmem, smem],
        out_specs=(hbm, vmem, vmem),
        scratch_shapes=[
            wide_vmem,
            wide_vmem,
            wide_vmem,
            pltpu.VMEM((WIDE, 16, NY), f32),
            slab_vmem,
            pltpu.VMEM((160, 128), f32),
            pltpu.VMEM((6, 2, 160, 128), f32),
            pltpu.VMEM((128, 128), f32),
            dma,
            dma((3, M)),
            dma((ROWS // 8, ZL)),
        ],
        compiler_params=pltpu.CompilerParams(vmem_limit_bytes=40 << 20),
    )(
        parts,
        on_hbm(warm),
        shapes,
        on_hbm(above),
        on_hbm(below),
        jnp.asarray(selection(16, 160)),
        injected_coefficients,
    )
    parts = lax.all_to_all(packed, "rows", 0, 0, tiled=True)
    refreshed = pl.pallas_call(
        spread,
        name="spread",
        out_shape=jax.ShapeDtypeStruct((M, ZL, M), f32),
        in_specs=[vmem, vmem],
        out_specs=vmem,
        compiler_params=pltpu.CompilerParams(vmem_limit_bytes=8 << 20),
    )(parts, jnp.asarray(selection(M, 128)))
    return (field, jnp.transpose(refreshed, (1, 0, 2)), jnp.transpose(incoming, (2, 1, 0)))


def solution(mesh):
    placed = (P("gz", "rows", None), P(None, "rows", None), P("gz", None), P())
    return jax.shard_map(
        shards,
        mesh=mesh,
        in_specs=placed,
        out_specs=(P("gz", "rows", None), P("gz", None, None), P("gz", None, None)),
        check_vma=False,
    )
```

```python
import jax
import jax.numpy as jnp
import numpy as np
from jax import lax
from jax.experimental import pallas as pl
from jax.experimental.pallas import tpu as pltpu
from jax.sharding import PartitionSpec as P

NX = 1024
NY = 1024
M = 10
PASSES = 16
ROWS = 32
HALO = 16
WIDE = ROWS + 2 * HALO
ZL = 16
GZ = 4
TILES = NY // 128
BLOCK = 8
TALL = WIDE + BLOCK
CHUNKS = 4
highest = lax.Precision.HIGHEST
f32 = jnp.float32
bf16 = jnp.bfloat16


def pair_modes():
    table = []
    for group in range(8):
        for sub in range(8):
            if group < 3:
                table.append((group, sub))
            elif group == 3:
                table.append(((8, 8), (8, 9), (9, 9))[sub] if sub < 3 else (3, sub))
            elif group < 6:
                first = 4 + 2 * (group - 4)
                table.append((first, 4 + sub) if sub < 4 else (first + 1, sub))
            else:
                table.append((group + 2, sub))
    return table


def selection(stride, rows):
    where = {}
    for row, (m, n) in enumerate(pair_modes()):
        where.setdefault((m, n), row)
        where.setdefault((n, m), row)
    chosen = np.zeros((rows, 64), np.float32)
    for i in range(M):
        for j in range(M):
            chosen[i * stride + j, where[(i, j)]] = 1.0
    return chosen


def diagonal_rows():
    table = pair_modes()
    return [table.index((m, m)) for m in range(M)]


def split(value):
    high = value.astype(bf16)
    low = (value - high.astype(f32)).astype(bf16)
    return high, low


def pair_products(modes_ref, row):
    low = modes_ref[row, 0:8, :]
    sub = lax.broadcasted_iota(jnp.int32, (8, NY), 0)

    def mode(m):
        return jnp.broadcast_to(modes_ref[row, m : m + 1, :], (8, NY))

    m8, m9 = mode(8), mode(9)
    turned = jnp.where(sub < 4, pltpu.roll(low, 4, 0), low)
    left3 = jnp.where(sub < 2, m8, jnp.where(sub == 2, m9, mode(3)))
    right3 = jnp.where(sub == 0, m8, jnp.where(sub < 3, m9, low))
    groups = [
        mode(0) * low,
        mode(1) * low,
        mode(2) * low,
        left3 * right3,
        jnp.where(sub < 4, mode(4), mode(5)) * turned,
        jnp.where(sub < 4, mode(6), mode(7)) * turned,
        m8 * low,
        m9 * low,
    ]
    return jnp.concatenate(groups, axis=0)


def sums_of_rows(field_ref, first, modes_ref, modes_first, count, unroll, start):
    def step(r, acc):
        products = jnp.concatenate(split(pair_products(modes_ref, modes_first + r)), axis=0)
        warmth = jnp.concatenate(split(field_ref[first + r]), axis=0)
        return acc + lax.dot_general(
            products, warmth, (((1,), (1,)), ((), ())), preferred_element_type=f32
        )

    return lax.fori_loop(0, count, step, start, unroll=unroll)


def packed_sums(acc, pad_ref, scale, extra):
    pad_ref[...] = jnp.zeros((128, 128), f32)
    pad_ref[:, 0:32] = acc
    both = pad_ref[0:64, :] + pad_ref[64:128, :]
    total = (both + pltpu.roll(both, 112, 1)) * scale
    lane = lax.broadcasted_iota(jnp.int32, (64, 128), 1)
    total = jnp.where(lane < ZL, total, 0.0)
    if extra is not None:
        total = total + extra
    packed = total[0:8]
    for group in range(1, 8):
        packed = packed + pltpu.roll(total[8 * group : 8 * group + 8], 16 * group, 1)
    return packed


def cut_edges(w, e, low, high, raw, lsem, ssem):
    groups = ((w.at[0:8], 0, 8), (w.at[8:16], 8, 8), (e, 16, 10))
    loads, stores = [], []
    for i, (origin, start, count) in enumerate(groups):
        at = slice(start, start + count)
        loads.append(pltpu.make_async_copy(origin, raw.at[at], lsem.at[i]))
        loads[i].start()
        stores += [
            pltpu.make_async_copy(raw.at[at, ROWS - HALO : ROWS, :], low.at[at], ssem.at[i, 0]),
            pltpu.make_async_copy(raw.at[at, 0:HALO, :], high.at[at], ssem.at[i, 1]),
        ]
    for i in range(3):
        loads[i].wait()
        for copy in stores[2 * i : 2 * i + 2]:
            copy.start()
    for copy in stores:
        copy.wait()


def spots(k):
    return pl.ds(64 * (k % 2) + k // 2, 8, stride=8)


def turn_in(value, new, row):
    stacked = jnp.concatenate([value[:, 128 * t : 128 * t + 128] for t in range(TILES)], axis=0)
    across = stacked.T
    for k in range(16):
        new[row, spots(k), :] = across[8 * k : 8 * k + 8]


def turn_out(old, row, new, new_row):
    across = jnp.concatenate([old[row, spots(k), :] for k in range(16)], axis=0).T
    for t in range(TILES):
        new[new_row, :, 128 * t : 128 * t + 128] = across[16 * t : 16 * t + 16]


def turn_slab(loads, raw, er, new, warm, modes, ssem):
    er[:, 8:16, :] = jnp.zeros((ROWS, 8, NY), f32)
    stores = [
        pltpu.make_async_copy(er, modes, ssem.at[0]),
        pltpu.make_async_copy(new, warm, ssem.at[1]),
    ]
    for copies in loads:
        for copy in copies:
            copy.start()
    for part, copies in enumerate(loads[:-1]):
        for copy in copies:
            copy.wait()

        def step(r, unused):
            turn_in(raw[HALO * part + r], new, HALO * part + r)
            return unused

        lax.fori_loop(0, HALO, step, 0, unroll=8)
    stores[1].start()
    for copy in loads[-1]:
        copy.wait()
    stores[0].start()
    for copy in stores:
        copy.wait()


def turn_edges(above, below, warm, modes, raw, er, new, lsem, msem, ssem):
    loads, mode_loads = [], []
    for side, edge in enumerate((above, below)):
        at = slice(HALO * side, HALO * side + HALO)
        loads.append(
            [
                pltpu.make_async_copy(edge.at[z], raw.at[at, z, :], lsem.at[side, z])
                for z in range(ZL)
            ]
        )
        mode_loads += [
            pltpu.make_async_copy(edge.at[ZL + m], er.at[at, m, :], msem.at[side, m])
            for m in range(M)
        ]
    turn_slab(loads + [mode_loads], raw, er, new, warm, modes, ssem)


def start_sums(
    w, e, ph, unused_low, out, warm, modes, wt, et, tw, pad, phv, wsem, esem, psem, ssem
):
    count = ROWS // CHUNKS
    chunks, stores = [], []
    for part in range(CHUNKS):
        at = slice(count * part, count * (part + 1))
        chunks.append(
            [
                pltpu.make_async_copy(w.at[z, at, :], wt.at[at, z, :], wsem.at[part, z])
                for z in range(ZL)
            ]
            + [
                pltpu.make_async_copy(e.at[m, at, :], et.at[at, m, :], esem.at[part, m])
                for m in range(M)
            ]
        )
        stores.append(
            [
                pltpu.make_async_copy(et.at[at], modes.at[at], ssem.at[part, 0]),
                pltpu.make_async_copy(tw.at[at], warm.at[at], ssem.at[part, 1]),
            ]
        )
    et[:, 8:16, :] = jnp.zeros((ROWS, 8, NY), f32)
    for copies in chunks:
        for copy in copies:
            copy.start()
    phase_copy = pltpu.make_async_copy(ph, phv, psem)
    phase_copy.start()
    acc = jnp.zeros((128, 32), f32)
    for part, copies in enumerate(chunks):
        for copy in copies:
            copy.wait()
        stores[part][0].start()
        start = count * part
        for r in range(start, start + count):
            turn_in(wt[r], tw, r)
        acc = sums_of_rows(wt, start, et, start, count, count, acc)
        stores[part][1].start()
    phase_copy.wait()
    pad[...] = jnp.zeros((128, 128), f32)
    pad[0:ZL, 0:M] = phv[...]
    turned = pad[...].T
    row = lax.broadcasted_iota(jnp.int32, (64, 128), 0)
    phases = jnp.zeros((64, 128), f32)
    for m, place in enumerate(diagonal_rows()):
        phases = phases + jnp.where(
            row == place, jnp.broadcast_to(turned[m : m + 1, :], (64, 128)), 0.0
        )
    phases = phases * jnp.where(lax.axis_index("rows") == 0, 1.0, 0.0)
    out[...] = packed_sums(acc, pad, 2.0 / float(NX * NY), phases)
    for copies in stores:
        for copy in copies:
            copy.wait()


def row_of(ref, *index):
    return jnp.broadcast_to(ref[index], (16, 128))


def amplitudes(parts, pick, v0, cs, ts, square, incoming):
    lane8 = lax.broadcasted_iota(jnp.int32, (8, 128), 1)
    totals = []
    for q in range(GZ):
        total = parts[q]
        for r in range(1, parts.shape[0] // GZ):
            total = total + parts[GZ * r + q]
        totals.append(total)
    rows = []
    for group in range(8):
        merged = jnp.zeros((8, 128), f32)
        for q in range(GZ):
            moved = pltpu.roll(totals[q], (16 * q - 16 * group) % 128, 1)
            merged = jnp.where(lane8 // ZL == q, moved, merged)
        rows.append(merged)
    pairs = jnp.concatenate(rows, axis=0)
    cs[...] = jnp.dot(pick[...], pairs, precision=highest, preferred_element_type=f32)

    sub = lax.broadcasted_iota(jnp.int32, (16, 128), 0)
    lane = lax.broadcasted_iota(jnp.int32, (16, 128), 1)
    coupled = [cs[16 * i : 16 * i + 16, :] for i in range(M)]
    matrix = []
    right = []
    for i in range(M):
        total = jnp.where(sub == i, 1.0, 0.0)
        for k in range(M):
            total = total + row_of(cs, pl.ds(16 * i + k, 1), slice(None)) * coupled[k]
        matrix.append(total)
        right.append(2.0 * coupled[i])
    for k in range(M):
        pivot = 1.0 / matrix[k][k : k + 1, :]
        pivot = jnp.broadcast_to(pivot, (16, 128))
        row_m = jnp.where(sub == k, pivot, matrix[k] * pivot)
        row_b = right[k] * pivot
        for i in range(M):
            if i != k:
                factor = jnp.broadcast_to(matrix[i][k : k + 1, :], (16, 128))
                matrix[i] = jnp.where(sub == k, 0.0, matrix[i]) - factor * row_m
                right[i] = right[i] - factor * row_b
        matrix[k] = row_m
        right[k] = row_b
    for i in range(M):
        ts[0, 0, 16 * i : 16 * i + 16, :] = 2.0 * matrix[i] - jnp.where(sub == i, 1.0, 0.0)
        ts[0, 1, 16 * i : 16 * i + 16, :] = right[i]

    for level in range(1, 6):
        back = 128 - (1 << (level - 1))
        later_r = [
            pltpu.roll(ts[level - 1, 0, 16 * j : 16 * j + 16, :], back, 1) for j in range(M)
        ]
        later_i = [
            pltpu.roll(ts[level - 1, 1, 16 * j : 16 * j + 16, :], back, 1) for j in range(M)
        ]
        for k in range(M):
            real = jnp.zeros((16, 128), f32)
            imag = jnp.zeros((16, 128), f32)
            for j in range(M):
                er = row_of(ts, level - 1, 0, pl.ds(16 * k + j, 1), slice(None))
                ei = row_of(ts, level - 1, 1, pl.ds(16 * k + j, 1), slice(None))
                real = real + (er * later_r[j] - ei * later_i[j])
                imag = imag + (er * later_i[j] + ei * later_r[j])
            ts[level, 0, 16 * k : 16 * k + 16, :] = real
            ts[level, 1, 16 * k : 16 * k + 16, :] = imag

    vr = jnp.zeros((16, 128), f32)
    vi = jnp.zeros((16, 128), f32)
    for m in range(M):
        spot = (sub == m) & (lane == 0)
        vr = jnp.where(spot, v0[0, m], vr)
        vi = jnp.where(spot, v0[1, m], vi)
    for level in range(5, -1, -1):
        half = 1 << level
        yr = jnp.zeros((16, 128), f32)
        yi = jnp.zeros((16, 128), f32)
        for k in range(M):
            tr = ts[level, 0, 16 * k : 16 * k + 16, :]
            ti = ts[level, 1, 16 * k : 16 * k + 16, :]
            ar = jnp.broadcast_to(vr[k : k + 1, :], (16, 128))
            ai = jnp.broadcast_to(vi[k : k + 1, :], (16, 128))
            yr = yr + (tr * ar - ti * ai)
            yi = yi + (tr * ai + ti * ar)
        target = lane % (2 * half) == half
        vr = jnp.where(target, pltpu.roll(yr, half, 1), vr)
        vi = jnp.where(target, pltpu.roll(yi, half, 1), vi)

    turn = (128 - ZL * lax.axis_index("gz")) % 128
    square[...] = jnp.zeros((128, 128), f32)
    vr = pltpu.roll(vr, turn, 1)
    vi = pltpu.roll(vi, turn, 1)
    incoming[:, 0, :] = vr[0:M, 0:ZL]
    incoming[:, 1, :] = vi[0:M, 0:ZL]
    square[0:16, :] = vr
    square[16:32, :] = vi
    turned = square[...].T[0:ZL, :]
    real = jnp.where(lane < 16, turned, 0.0)
    imag = jnp.where(lane < 16, pltpu.roll(turned, 112, 1), 0.0)
    return real, imag


def heat_load(real, imag, modes_ref, source_ref):
    both = jnp.concatenate([real, imag], axis=0)
    high = both.astype(bf16).astype(f32)
    low = both - high
    weights = high + pltpu.roll(high, 16, 1) + pltpu.roll(low, 32, 1) + pltpu.roll(low, 48, 1)
    weights = weights[:, 0:64].astype(bf16)

    def step(r, unused):
        high_e, low_e = split(modes_ref[r])
        stacked = jnp.concatenate([high_e, low_e, high_e, low_e], axis=0)
        field = jnp.dot(weights, stacked, preferred_element_type=f32)
        re, im = field[0:16], field[16:32]
        turn_in(0.01 * (re * re + im * im), source_ref, r)
        return unused

    lax.fori_loop(0, WIDE, step, 0, unroll=16)


def one_pass(old, new, source, number):
    lane = lax.broadcasted_iota(jnp.int32, (8, 128), 1)
    sub = lax.broadcasted_iota(jnp.int32, (8, 128), 0)

    def block(b, unused):
        r = number + BLOCK * b
        for half in range(2):
            some = range(8 * half, 8 * half + 8)

            def register(row, v):
                return old[row, 8 * v : 8 * v + 8, :]

            rows = [{v: register(r - 1 + i, v) for v in some} for i in range(BLOCK + 2)]
            for i in range(BLOCK):
                center = dict(rows[i + 1])
                if half == 0:
                    near = pltpu.roll(register(r + i, 15), 1, 0)
                    far = jnp.where(lane < 16, 0.0, pltpu.roll(near, 16, 1))
                    center[-1] = jnp.where(sub == 0, far, near)
                    center[8] = register(r + i, 8)
                else:
                    near = pltpu.roll(register(r + i, 0), 7, 0)
                    far = jnp.where(lane >= 112, 0.0, pltpu.roll(near, 112, 1))
                    center[16] = jnp.where(sub == 7, far, near)
                    center[7] = register(r + i, 7)
                for v in some:
                    sides = center[v - 1] + center[v + 1]
                    total = (rows[i][v] + center[v]) + (rows[i + 2][v] + sides)
                    cut = slice(8 * v, 8 * v + 8)
                    new[r + i, cut, :] = 0.2 * total + source[r + i, cut, :]
        return unused

    lax.fori_loop(0, (WIDE - 2 * number + BLOCK - 1) // BLOCK, block, 0)


def heat_and_sums(
    parts, warm, modes, edge_warm, edge_modes, pick, v0,
    field, out, incoming,
    f0, f1, source, et, plain, cs, ts, square, wsem, esem, osem,
):
    own = slice(HALO, HALO + ROWS)
    above, below = slice(0, HALO), slice(HALO + ROWS, WIDE)
    mode_copies, copies = [
        [
            pltpu.make_async_copy(inner, wide.at[own], sem.at[0]),
            pltpu.make_async_copy(outer.at[0:HALO], wide.at[above], sem.at[1]),
            pltpu.make_async_copy(outer.at[HALO : 2 * HALO], wide.at[below], sem.at[2]),
        ]
        for inner, outer, wide, sem in (
            (modes, edge_modes, et, esem),
            (warm, edge_warm, f0, wsem),
        )
    ]
    for copy in mode_copies:
        copy.start()
    real, imag = amplitudes(parts, pick, v0, cs, ts, square, incoming)
    for copy in mode_copies:
        copy.wait()
    for copy in copies:
        copy.start()
    heat_load(real, imag, et, source)
    for copy in copies:
        copy.wait()
    place = lax.axis_index("rows")
    first = place == 0
    last = place == lax.axis_size("rows") - 1
    buffers = (f0, f1)
    for number in range(1, PASSES + 1):
        old, new = buffers[(number - 1) % 2], buffers[number % 2]
        one_pass(old, new, source, number)
        if number < PASSES:

            @pl.when(first)
            def _():
                new[HALO - 1] = jnp.zeros((128, 128), f32)

            @pl.when(last)
            def _():
                new[HALO + ROWS] = jnp.zeros((128, 128), f32)

    done = buffers[PASSES % 2]
    outs = []
    for part in range(ROWS // 8):
        at = slice(8 * part, 8 * part + 8)
        for r in range(8 * part, 8 * part + 8):
            turn_out(done, HALO + r, plain, r)
        for z in range(ZL):
            copy = pltpu.make_async_copy(plain.at[at, z, :], field.at[z, at, :], osem.at[part, z])
            copy.start()
            outs.append(copy)
    acc = sums_of_rows(plain, 0, et, HALO, ROWS, 16, jnp.zeros((128, 32), f32))
    packed = packed_sums(acc, square, 1.0 / float(NX * NY), None)
    out[...] = jnp.broadcast_to(packed[None], out.shape)
    for copy in outs:
        copy.wait()


def spread(parts, pick, out):
    total = parts[0]
    for r in range(1, parts.shape[0]):
        total = total + parts[r]
    rows = [total] + [pltpu.roll(total, 128 - 16 * group, 1) for group in range(1, 8)]
    pairs = jnp.concatenate(rows, axis=0)
    table = jnp.dot(pick[...], pairs, precision=highest, preferred_element_type=f32).T
    for m in range(M):
        out[m] = table[0:ZL, M * m : M * m + M]


def on_hbm(array):
    return pltpu.with_memory_space_constraint(array, pltpu.HBM)


def shards(segment_warming, eigenfunction_crosssections, segment_phasors, injected_coefficients):
    devices = lax.axis_size("rows")
    hbm = pl.BlockSpec(memory_space=pltpu.HBM)
    vmem = pl.BlockSpec(memory_space=pltpu.VMEM)
    smem = pl.BlockSpec(memory_space=pltpu.SMEM)
    dma = pltpu.SemaphoreType.DMA
    edge = pltpu.HBM((ZL + M, HALO, NY), f32)
    slab_vmem = pltpu.VMEM((ROWS, 16, NY), f32)
    warming, shapes = on_hbm(segment_warming), on_hbm(eigenfunction_crosssections)
    low, high = pl.pallas_call(
        cut_edges,
        name="cut_edges",
        out_shape=(edge, edge),
        in_specs=[hbm, hbm],
        out_specs=(hbm, hbm),
        scratch_shapes=[pltpu.VMEM((ZL + M, ROWS, NY), f32), dma((3,)), dma((3, 2))],
        compiler_params=pltpu.CompilerParams(vmem_limit_bytes=16 << 20),
    )(warming, shapes)
    forward = [(i, i + 1) for i in range(devices - 1)]
    backward = [(target, origin) for origin, target in forward]
    slab = (pltpu.HBM((ROWS, 128, 128), f32), pltpu.HBM((ROWS, 16, NY), f32))
    packed, warm, modes = pl.pallas_call(
        start_sums,
        name="start_sums",
        out_shape=(jax.ShapeDtypeStruct((8, 128), f32),) + slab,
        in_specs=[hbm, hbm, hbm, hbm],
        out_specs=(vmem, hbm, hbm),
        scratch_shapes=[
            slab_vmem,
            slab_vmem,
            pltpu.VMEM((ROWS, 128, 128), f32),
            pltpu.VMEM((128, 128), f32),
            pltpu.VMEM((ZL, M), f32),
            dma((CHUNKS, ZL)),
            dma((CHUNKS, M)),
            dma,
            dma((CHUNKS, 2)),
        ],
        compiler_params=pltpu.CompilerParams(vmem_limit_bytes=24 << 20),
    )(warming, shapes, on_hbm(segment_phasors), on_hbm(low))
    mate = lax.ppermute(packed, "rows", [(i, i ^ 1) for i in range(devices)])
    above = lax.ppermute(low, "rows", forward)
    below = lax.ppermute(high, "rows", backward)
    both = jnp.broadcast_to((packed + mate)[None], (devices * GZ // 2, 8, 128))
    groups = [
        [GZ * (2 * chip + core) + q for chip in range(devices // 2) for q in range(GZ)]
        for core in range(2)
    ]
    parts = lax.all_to_all(
        both, ("rows", "gz"), 0, 0, axis_index_groups=groups, tiled=True
    )
    turn_scratch = [slab_vmem, slab_vmem, pltpu.VMEM((ROWS, 128, 128), f32)]
    edge_warm, edge_modes = pl.pallas_call(
        turn_edges,
        name="turn_edges",
        out_shape=slab,
        in_specs=[hbm, hbm],
        out_specs=(hbm, hbm),
        scratch_shapes=turn_scratch + [dma((2, ZL)), dma((2, M)), dma((2,))],
        compiler_params=pltpu.CompilerParams(vmem_limit_bytes=16 << 20),
    )(on_hbm(above), on_hbm(below))
    wide_vmem = pltpu.VMEM((TALL, 128, 128), f32)
    field, packed, incoming = pl.pallas_call(
        heat_and_sums,
        name="heat_and_sums",
        out_shape=(
            jax.ShapeDtypeStruct((ZL, ROWS, NY), f32),
            jax.ShapeDtypeStruct((devices, 8, 128), f32),
            jax.ShapeDtypeStruct((M, 2, ZL), f32),
        ),
        in_specs=[vmem, hbm, hbm, hbm, hbm, vmem, smem],
        out_specs=(hbm, vmem, vmem),
        scratch_shapes=[
            wide_vmem,
            wide_vmem,
            wide_vmem,
            pltpu.VMEM((WIDE, 16, NY), f32),
            slab_vmem,
            pltpu.VMEM((160, 128), f32),
            pltpu.VMEM((6, 2, 160, 128), f32),
            pltpu.VMEM((128, 128), f32),
            dma((3,)),
            dma((3,)),
            dma((ROWS // 8, ZL)),
        ],
        compiler_params=pltpu.CompilerParams(vmem_limit_bytes=40 << 20),
    )(
        parts,
        on_hbm(warm),
        on_hbm(modes),
        on_hbm(edge_warm),
        on_hbm(edge_modes),
        jnp.asarray(selection(16, 160)),
        injected_coefficients,
    )
    parts = lax.all_to_all(packed, "rows", 0, 0, tiled=True)
    refreshed = pl.pallas_call(
        spread,
        name="spread",
        out_shape=jax.ShapeDtypeStruct((M, ZL, M), f32),
        in_specs=[vmem, vmem],
        out_specs=vmem,
        compiler_params=pltpu.CompilerParams(vmem_limit_bytes=8 << 20),
    )(parts, jnp.asarray(selection(M, 128)))
    return (field, jnp.transpose(refreshed, (1, 0, 2)), jnp.transpose(incoming, (2, 1, 0)))


def solution(mesh):
    placed = (P("gz", "rows", None), P(None, "rows", None), P("gz", None), P())
    return jax.shard_map(
        shards,
        mesh=mesh,
        in_specs=placed,
        out_specs=(P("gz", "rows", None), P("gz", None, None), P("gz", None, None)),
        check_vma=False,
    )
```

```python
import jax
import jax.numpy as jnp
import numpy as np
from jax import lax
from jax.experimental import pallas as pl
from jax.experimental.pallas import tpu as pltpu
from jax.sharding import PartitionSpec as P

NX = 1024
NY = 1024
M = 10
PASSES = 16
ROWS = 32
HALO = 16
WIDE = ROWS + 2 * HALO
ZL = 16
GZ = 4
TILES = NY // 128
BLOCK = 8
TALL = WIDE + BLOCK
CHUNKS = 4
highest = lax.Precision.HIGHEST
f32 = jnp.float32
bf16 = jnp.bfloat16


def pair_modes():
    table = []
    for group in range(8):
        for sub in range(8):
            if group < 3:
                table.append((group, sub))
            elif group == 3:
                table.append(((8, 8), (8, 9), (9, 9))[sub] if sub < 3 else (3, sub))
            elif group < 6:
                first = 4 + 2 * (group - 4)
                table.append((first, 4 + sub) if sub < 4 else (first + 1, sub))
            else:
                table.append((group + 2, sub))
    return table


def selection(stride, rows):
    where = {}
    for row, (m, n) in enumerate(pair_modes()):
        where.setdefault((m, n), row)
        where.setdefault((n, m), row)
    chosen = np.zeros((rows, 64), np.float32)
    for i in range(M):
        for j in range(M):
            chosen[i * stride + j, where[(i, j)]] = 1.0
    return chosen


def diagonal_rows():
    table = pair_modes()
    return [table.index((m, m)) for m in range(M)]


def split(value):
    high = value.astype(bf16)
    low = (value - high.astype(f32)).astype(bf16)
    return high, low


def pair_products(modes_ref, row):
    low = modes_ref[row, 0:8, :]
    sub = lax.broadcasted_iota(jnp.int32, (8, NY), 0)

    def mode(m):
        return jnp.broadcast_to(modes_ref[row, m : m + 1, :], (8, NY))

    m8, m9 = mode(8), mode(9)
    turned = jnp.where(sub < 4, pltpu.roll(low, 4, 0), low)
    left3 = jnp.where(sub < 2, m8, jnp.where(sub == 2, m9, mode(3)))
    right3 = jnp.where(sub == 0, m8, jnp.where(sub < 3, m9, low))
    groups = [
        mode(0) * low,
        mode(1) * low,
        mode(2) * low,
        left3 * right3,
        jnp.where(sub < 4, mode(4), mode(5)) * turned,
        jnp.where(sub < 4, mode(6), mode(7)) * turned,
        m8 * low,
        m9 * low,
    ]
    return jnp.concatenate(groups, axis=0)


def sums_of_rows(field_ref, first, modes_ref, modes_first, count, unroll, start):
    def step(r, acc):
        products = jnp.concatenate(split(pair_products(modes_ref, modes_first + r)), axis=0)
        warmth = jnp.concatenate(split(field_ref[first + r]), axis=0)
        return acc + lax.dot_general(
            products, warmth, (((1,), (1,)), ((), ())), preferred_element_type=f32
        )

    return lax.fori_loop(0, count, step, start, unroll=unroll)


def packed_sums(acc, pad_ref, scale, extra):
    pad_ref[...] = jnp.zeros((128, 128), f32)
    pad_ref[:, 0:32] = acc
    both = pad_ref[0:64, :] + pad_ref[64:128, :]
    total = (both + pltpu.roll(both, 112, 1)) * scale
    lane = lax.broadcasted_iota(jnp.int32, (64, 128), 1)
    total = jnp.where(lane < ZL, total, 0.0)
    if extra is not None:
        total = total + extra
    packed = total[0:8]
    for group in range(1, 8):
        packed = packed + pltpu.roll(total[8 * group : 8 * group + 8], 16 * group, 1)
    return packed


def cut_edges(w, e, low, high, raw, lsem, ssem):
    groups = ((w.at[0:8], 0, 8), (w.at[8:16], 8, 8), (e, 16, 10))
    loads, stores = [], []
    for i, (origin, start, count) in enumerate(groups):
        at = slice(start, start + count)
        loads.append(pltpu.make_async_copy(origin, raw.at[at], lsem.at[i]))
        loads[i].start()
        stores += [
            pltpu.make_async_copy(raw.at[at, ROWS - HALO : ROWS, :], low.at[at], ssem.at[i, 0]),
            pltpu.make_async_copy(raw.at[at, 0:HALO, :], high.at[at], ssem.at[i, 1]),
        ]
    for i in range(3):
        loads[i].wait()
        for copy in stores[2 * i : 2 * i + 2]:
            copy.start()
    for copy in stores:
        copy.wait()


def spots(k):
    return pl.ds(64 * (k % 2) + k // 2, 8, stride=8)


def turn_in(value, new, row):
    stacked = jnp.concatenate([value[:, 128 * t : 128 * t + 128] for t in range(TILES)], axis=0)
    across = stacked.T
    for k in range(16):
        new[row, spots(k), :] = across[8 * k : 8 * k + 8]


def turn_out(old, row, new, new_row):
    across = jnp.concatenate([old[row, spots(k), :] for k in range(16)], axis=0).T
    for t in range(TILES):
        new[new_row, :, 128 * t : 128 * t + 128] = across[16 * t : 16 * t + 16]


def turn_slab(loads, raw, er, new, warm, modes, ssem):
    er[:, 8:16, :] = jnp.zeros((ROWS, 8, NY), f32)
    stores = [
        pltpu.make_async_copy(er, modes, ssem.at[0]),
        pltpu.make_async_copy(new, warm, ssem.at[1]),
    ]
    for copies in loads:
        for copy in copies:
            copy.start()
    for part, copies in enumerate(loads[:-1]):
        for copy in copies:
            copy.wait()

        def step(r, unused):
            turn_in(raw[HALO * part + r], new, HALO * part + r)
            return unused

        lax.fori_loop(0, HALO, step, 0, unroll=8)
    stores[1].start()
    for copy in loads[-1]:
        copy.wait()
    stores[0].start()
    for copy in stores:
        copy.wait()


def turn_edges(above, below, warm, modes, raw, er, new, lsem, msem, ssem):
    loads, mode_loads = [], []
    for side, edge in enumerate((above, below)):
        at = slice(HALO * side, HALO * side + HALO)
        loads.append(
            [
                pltpu.make_async_copy(edge.at[z], raw.at[at, z, :], lsem.at[side, z])
                for z in range(ZL)
            ]
        )
        mode_loads += [
            pltpu.make_async_copy(edge.at[ZL + m], er.at[at, m, :], msem.at[side, m])
            for m in range(M)
        ]
    turn_slab(loads + [mode_loads], raw, er, new, warm, modes, ssem)


def start_sums(
    w, e, ph, unused_low, out, warm, modes, wt, et, tw, pad, phv, wsem, esem, psem, ssem
):
    count = ROWS // CHUNKS
    chunks, stores = [], []
    for part in range(CHUNKS):
        at = slice(count * part, count * (part + 1))
        chunks.append(
            [
                pltpu.make_async_copy(w.at[z, at, :], wt.at[at, z, :], wsem.at[part, z])
                for z in range(ZL)
            ]
            + [
                pltpu.make_async_copy(e.at[m, at, :], et.at[at, m, :], esem.at[part, m])
                for m in range(M)
            ]
        )
        stores.append(
            [
                pltpu.make_async_copy(et.at[at], modes.at[at], ssem.at[part, 0]),
                pltpu.make_async_copy(tw.at[at], warm.at[at], ssem.at[part, 1]),
            ]
        )
    et[:, 8:16, :] = jnp.zeros((ROWS, 8, NY), f32)
    phase_copy = pltpu.make_async_copy(ph, phv, psem)
    phase_copy.start()
    for copies in chunks:
        for copy in copies:
            copy.start()
    phase_copy.wait()
    pad[...] = jnp.zeros((128, 128), f32)
    pad[0:ZL, 0:M] = phv[...]
    turned = pad[...].T
    row = lax.broadcasted_iota(jnp.int32, (64, 128), 0)
    phases = jnp.zeros((64, 128), f32)
    for m, place in enumerate(diagonal_rows()):
        phases = phases + jnp.where(
            row == place, jnp.broadcast_to(turned[m : m + 1, :], (64, 128)), 0.0
        )
    phases = phases * jnp.where(lax.axis_index("rows") == 0, 1.0, 0.0)
    acc = jnp.zeros((128, 32), f32)
    for part, copies in enumerate(chunks):
        for copy in copies:
            copy.wait()
        stores[part][0].start()
        start = count * part
        for r in range(start, start + count):
            turn_in(wt[r], tw, r)
        acc = sums_of_rows(wt, start, et, start, count, count, acc)
        stores[part][1].start()
    out[...] = packed_sums(acc, pad, 2.0 / float(NX * NY), phases)
    for copies in stores:
        for copy in copies:
            copy.wait()


def row_of(ref, *index):
    return jnp.broadcast_to(ref[index], (16, 128))


def amplitudes(parts, pick, v0, cs, ts, square, incoming):
    lane8 = lax.broadcasted_iota(jnp.int32, (8, 128), 1)
    totals = []
    for q in range(GZ):
        total = parts[q]
        for r in range(1, parts.shape[0] // GZ):
            total = total + parts[GZ * r + q]
        totals.append(total)
    rows = []
    for group in range(8):
        merged = jnp.zeros((8, 128), f32)
        for q in range(GZ):
            moved = pltpu.roll(totals[q], (16 * q - 16 * group) % 128, 1)
            merged = jnp.where(lane8 // ZL == q, moved, merged)
        rows.append(merged)
    pairs = jnp.concatenate(rows, axis=0)
    cs[...] = jnp.dot(pick[...], pairs, precision=highest, preferred_element_type=f32)

    sub = lax.broadcasted_iota(jnp.int32, (16, 128), 0)
    lane = lax.broadcasted_iota(jnp.int32, (16, 128), 1)
    coupled = [cs[16 * i : 16 * i + 16, :] for i in range(M)]
    matrix = []
    right = []
    for i in range(M):
        total = jnp.where(sub == i, 1.0, 0.0)
        for k in range(M):
            total = total + row_of(cs, pl.ds(16 * i + k, 1), slice(None)) * coupled[k]
        matrix.append(total)
        right.append(2.0 * coupled[i])
    for k in range(M):
        pivot = 1.0 / matrix[k][k : k + 1, :]
        pivot = jnp.broadcast_to(pivot, (16, 128))
        row_m = jnp.where(sub == k, pivot, matrix[k] * pivot)
        row_b = right[k] * pivot
        for i in range(M):
            if i != k:
                factor = jnp.broadcast_to(matrix[i][k : k + 1, :], (16, 128))
                matrix[i] = jnp.where(sub == k, 0.0, matrix[i]) - factor * row_m
                right[i] = right[i] - factor * row_b
        matrix[k] = row_m
        right[k] = row_b
    for i in range(M):
        ts[0, 0, 16 * i : 16 * i + 16, :] = 2.0 * matrix[i] - jnp.where(sub == i, 1.0, 0.0)
        ts[0, 1, 16 * i : 16 * i + 16, :] = right[i]

    for level in range(1, 6):
        back = 128 - (1 << (level - 1))
        later_r = [
            pltpu.roll(ts[level - 1, 0, 16 * j : 16 * j + 16, :], back, 1) for j in range(M)
        ]
        later_i = [
            pltpu.roll(ts[level - 1, 1, 16 * j : 16 * j + 16, :], back, 1) for j in range(M)
        ]
        for k in range(M):
            real = jnp.zeros((16, 128), f32)
            imag = jnp.zeros((16, 128), f32)
            for j in range(M):
                er = row_of(ts, level - 1, 0, pl.ds(16 * k + j, 1), slice(None))
                ei = row_of(ts, level - 1, 1, pl.ds(16 * k + j, 1), slice(None))
                real = real + (er * later_r[j] - ei * later_i[j])
                imag = imag + (er * later_i[j] + ei * later_r[j])
            ts[level, 0, 16 * k : 16 * k + 16, :] = real
            ts[level, 1, 16 * k : 16 * k + 16, :] = imag

    vr = jnp.zeros((16, 128), f32)
    vi = jnp.zeros((16, 128), f32)
    for m in range(M):
        spot = (sub == m) & (lane == 0)
        vr = jnp.where(spot, v0[0, m], vr)
        vi = jnp.where(spot, v0[1, m], vi)
    for level in range(5, -1, -1):
        half = 1 << level
        yr = jnp.zeros((16, 128), f32)
        yi = jnp.zeros((16, 128), f32)
        for k in range(M):
            tr = ts[level, 0, 16 * k : 16 * k + 16, :]
            ti = ts[level, 1, 16 * k : 16 * k + 16, :]
            ar = jnp.broadcast_to(vr[k : k + 1, :], (16, 128))
            ai = jnp.broadcast_to(vi[k : k + 1, :], (16, 128))
            yr = yr + (tr * ar - ti * ai)
            yi = yi + (tr * ai + ti * ar)
        target = lane % (2 * half) == half
        vr = jnp.where(target, pltpu.roll(yr, half, 1), vr)
        vi = jnp.where(target, pltpu.roll(yi, half, 1), vi)

    turn = (128 - ZL * lax.axis_index("gz")) % 128
    square[...] = jnp.zeros((128, 128), f32)
    vr = pltpu.roll(vr, turn, 1)
    vi = pltpu.roll(vi, turn, 1)
    incoming[:, 0, :] = vr[0:M, 0:ZL]
    incoming[:, 1, :] = vi[0:M, 0:ZL]
    square[0:16, :] = vr
    square[16:32, :] = vi
    turned = square[...].T[0:ZL, :]
    real = jnp.where(lane < 16, turned, 0.0)
    imag = jnp.where(lane < 16, pltpu.roll(turned, 112, 1), 0.0)
    return real, imag


def heat_load(real, imag, modes_ref, source_ref):
    both = jnp.concatenate([real, imag], axis=0)
    high = both.astype(bf16).astype(f32)
    low = both - high
    weights = high + pltpu.roll(high, 16, 1) + pltpu.roll(low, 32, 1) + pltpu.roll(low, 48, 1)
    weights = weights[:, 0:64].astype(bf16)

    def step(r, unused):
        high_e, low_e = split(modes_ref[r])
        stacked = jnp.concatenate([high_e, low_e, high_e, low_e], axis=0)
        field = jnp.dot(weights, stacked, preferred_element_type=f32)
        re, im = field[0:16], field[16:32]
        turn_in(0.01 * (re * re + im * im), source_ref, r)
        return unused

    lax.fori_loop(0, WIDE, step, 0, unroll=16)


def one_pass(old, new, source, number):
    lane = lax.broadcasted_iota(jnp.int32, (8, 128), 1)
    sub = lax.broadcasted_iota(jnp.int32, (8, 128), 0)

    def block(b, unused):
        r = number + BLOCK * b
        for half in range(2):
            some = range(8 * half, 8 * half + 8)

            def register(row, v):
                return old[row, 8 * v : 8 * v + 8, :]

            rows = [{v: register(r - 1 + i, v) for v in some} for i in range(BLOCK + 2)]
            middle = {}
            for i in range(BLOCK):
                center = dict(rows[i + 1])
                if half == 0:
                    near = pltpu.roll(register(r + i, 15), 1, 0)
                    far = jnp.where(lane < 16, 0.0, pltpu.roll(near, 16, 1))
                    center[-1] = jnp.where(sub == 0, far, near)
                    center[8] = register(r + i, 8)
                else:
                    near = pltpu.roll(register(r + i, 0), 7, 0)
                    far = jnp.where(lane >= 112, 0.0, pltpu.roll(near, 112, 1))
                    center[16] = jnp.where(sub == 7, far, near)
                    center[7] = register(r + i, 7)
                for v in some:
                    sides = center[v - 1] + center[v + 1]
                    if i % 2 == 0:
                        middle[v] = center[v] + rows[i + 2][v]
                    outer = rows[i][v] if i % 2 == 0 else rows[i + 2][v]
                    total = (outer + middle[v]) + sides
                    cut = slice(8 * v, 8 * v + 8)
                    new[r + i, cut, :] = 0.2 * total + source[r + i, cut, :]
        return unused

    lax.fori_loop(0, (WIDE - 2 * number + BLOCK - 1) // BLOCK, block, 0)


def heat_and_sums(
    parts, warm, modes, edge_warm, edge_modes, pick, v0,
    field, out, incoming,
    f0, f1, source, et, plain, cs, ts, square, wsem, esem, osem,
):
    own = slice(HALO, HALO + ROWS)
    above, below = slice(0, HALO), slice(HALO + ROWS, WIDE)
    mode_copies, copies = [
        [
            pltpu.make_async_copy(inner, wide.at[own], sem.at[0]),
            pltpu.make_async_copy(outer.at[0:HALO], wide.at[above], sem.at[1]),
            pltpu.make_async_copy(outer.at[HALO : 2 * HALO], wide.at[below], sem.at[2]),
        ]
        for inner, outer, wide, sem in (
            (modes, edge_modes, et, esem),
            (warm, edge_warm, f0, wsem),
        )
    ]
    for copy in mode_copies:
        copy.start()
    real, imag = amplitudes(parts, pick, v0, cs, ts, square, incoming)
    for copy in mode_copies:
        copy.wait()
    for copy in copies:
        copy.start()
    heat_load(real, imag, et, source)
    for copy in copies:
        copy.wait()
    place = lax.axis_index("rows")
    first = place == 0
    last = place == lax.axis_size("rows") - 1
    buffers = (f0, f1)
    for number in range(1, PASSES + 1):
        old, new = buffers[(number - 1) % 2], buffers[number % 2]
        one_pass(old, new, source, number)
        if number < PASSES:

            @pl.when(first)
            def _():
                new[HALO - 1] = jnp.zeros((128, 128), f32)

            @pl.when(last)
            def _():
                new[HALO + ROWS] = jnp.zeros((128, 128), f32)

    done = buffers[PASSES % 2]
    outs = []
    for part in range(ROWS // 8):
        at = slice(8 * part, 8 * part + 8)
        for r in range(8 * part, 8 * part + 8):
            turn_out(done, HALO + r, plain, r)
        for z in range(ZL):
            copy = pltpu.make_async_copy(plain.at[at, z, :], field.at[z, at, :], osem.at[part, z])
            copy.start()
            outs.append(copy)
    acc = sums_of_rows(plain, 0, et, HALO, ROWS, 32, jnp.zeros((128, 32), f32))
    packed = packed_sums(acc, square, 1.0 / float(NX * NY), None)
    out[...] = jnp.broadcast_to(packed[None], out.shape)
    for copy in outs:
        copy.wait()


def spread(parts, pick, out):
    total = parts[0]
    for r in range(1, parts.shape[0]):
        total = total + parts[r]
    rows = [total] + [pltpu.roll(total, 128 - 16 * group, 1) for group in range(1, 8)]
    pairs = jnp.concatenate(rows, axis=0)
    table = jnp.dot(pick[...], pairs, precision=highest, preferred_element_type=f32).T
    for m in range(M):
        out[m] = table[0:ZL, M * m : M * m + M]


def on_hbm(array):
    return pltpu.with_memory_space_constraint(array, pltpu.HBM)


def shards(segment_warming, eigenfunction_crosssections, segment_phasors, injected_coefficients):
    devices = lax.axis_size("rows")
    hbm = pl.BlockSpec(memory_space=pltpu.HBM)
    vmem = pl.BlockSpec(memory_space=pltpu.VMEM)
    smem = pl.BlockSpec(memory_space=pltpu.SMEM)
    dma = pltpu.SemaphoreType.DMA
    edge = pltpu.HBM((ZL + M, HALO, NY), f32)
    slab_vmem = pltpu.VMEM((ROWS, 16, NY), f32)
    warming, shapes = on_hbm(segment_warming), on_hbm(eigenfunction_crosssections)
    low, high = pl.pallas_call(
        cut_edges,
        name="cut_edges",
        out_shape=(edge, edge),
        in_specs=[hbm, hbm],
        out_specs=(hbm, hbm),
        scratch_shapes=[pltpu.VMEM((ZL + M, ROWS, NY), f32), dma((3,)), dma((3, 2))],
        compiler_params=pltpu.CompilerParams(vmem_limit_bytes=16 << 20),
    )(warming, shapes)
    forward = [(i, i + 1) for i in range(devices - 1)]
    backward = [(target, origin) for origin, target in forward]
    slab = (pltpu.HBM((ROWS, 128, 128), f32), pltpu.HBM((ROWS, 16, NY), f32))
    packed, warm, modes = pl.pallas_call(
        start_sums,
        name="start_sums",
        out_shape=(jax.ShapeDtypeStruct((8, 128), f32),) + slab,
        in_specs=[hbm, hbm, hbm, hbm],
        out_specs=(vmem, hbm, hbm),
        scratch_shapes=[
            slab_vmem,
            slab_vmem,
            pltpu.VMEM((ROWS, 128, 128), f32),
            pltpu.VMEM((128, 128), f32),
            pltpu.VMEM((ZL, M), f32),
            dma((CHUNKS, ZL)),
            dma((CHUNKS, M)),
            dma,
            dma((CHUNKS, 2)),
        ],
        compiler_params=pltpu.CompilerParams(vmem_limit_bytes=24 << 20),
    )(warming, shapes, on_hbm(segment_phasors), on_hbm(low))
    mate = lax.ppermute(packed, "rows", [(i, i ^ 1) for i in range(devices)])
    above = lax.ppermute(low, "rows", forward)
    below = lax.ppermute(high, "rows", backward)
    both = jnp.broadcast_to((packed + mate)[None], (devices * GZ // 2, 8, 128))
    groups = [
        [GZ * (2 * chip + core) + q for chip in range(devices // 2) for q in range(GZ)]
        for core in range(2)
    ]
    parts = lax.all_to_all(
        both, ("rows", "gz"), 0, 0, axis_index_groups=groups, tiled=True
    )
    turn_scratch = [slab_vmem, slab_vmem, pltpu.VMEM((ROWS, 128, 128), f32)]
    edge_warm, edge_modes = pl.pallas_call(
        turn_edges,
        name="turn_edges",
        out_shape=slab,
        in_specs=[hbm, hbm],
        out_specs=(hbm, hbm),
        scratch_shapes=turn_scratch + [dma((2, ZL)), dma((2, M)), dma((2,))],
        compiler_params=pltpu.CompilerParams(vmem_limit_bytes=16 << 20),
    )(on_hbm(above), on_hbm(below))
    wide_vmem = pltpu.VMEM((TALL, 128, 128), f32)
    field, packed, incoming = pl.pallas_call(
        heat_and_sums,
        name="heat_and_sums",
        out_shape=(
            jax.ShapeDtypeStruct((ZL, ROWS, NY), f32),
            jax.ShapeDtypeStruct((devices, 8, 128), f32),
            jax.ShapeDtypeStruct((M, 2, ZL), f32),
        ),
        in_specs=[vmem, hbm, hbm, hbm, hbm, vmem, smem],
        out_specs=(hbm, vmem, vmem),
        scratch_shapes=[
            wide_vmem,
            wide_vmem,
            wide_vmem,
            pltpu.VMEM((WIDE, 16, NY), f32),
            slab_vmem,
            pltpu.VMEM((160, 128), f32),
            pltpu.VMEM((6, 2, 160, 128), f32),
            pltpu.VMEM((128, 128), f32),
            dma((3,)),
            dma((3,)),
            dma((ROWS // 8, ZL)),
        ],
        compiler_params=pltpu.CompilerParams(vmem_limit_bytes=40 << 20),
    )(
        parts,
        on_hbm(warm),
        on_hbm(modes),
        on_hbm(edge_warm),
        on_hbm(edge_modes),
        jnp.asarray(selection(16, 160)),
        injected_coefficients,
    )
    parts = lax.all_to_all(packed, "rows", 0, 0, tiled=True)
    refreshed = pl.pallas_call(
        spread,
        name="spread",
        out_shape=jax.ShapeDtypeStruct((M, ZL, M), f32),
        in_specs=[vmem, vmem],
        out_specs=vmem,
        compiler_params=pltpu.CompilerParams(vmem_limit_bytes=8 << 20),
    )(parts, jnp.asarray(selection(M, 128)))
    return (field, jnp.transpose(refreshed, (1, 0, 2)), jnp.transpose(incoming, (2, 1, 0)))


def solution(mesh):
    placed = (P("gz", "rows", None), P(None, "rows", None), P("gz", None), P())
    return jax.shard_map(
        shards,
        mesh=mesh,
        in_specs=placed,
        out_specs=(P("gz", "rows", None), P("gz", None, None), P("gz", None, None)),
        check_vma=False,
    )
```
